256 devices in a mesh: px: 2 (over core), py: 8 (over z), ta: 16 (over y, x).
Axes of the slice: x: 4, y: 4, z: 8, core: 2. Of those that a mesh axis runs over, the one named last changes fastest.
Arguments:
- snapshots: bfloat16 [384, 5, 131072], P('ta', None, ('px', 'py')), may hold values from -6 to 6
- quad_weights: float32 [131072], P(('px', 'py')), may hold values from 1 to 10
- spectral_indices: int32 [32], replicated, may hold values from 0 to 127
Outputs:
- spectra: float32 [32, 2, 2, 5, 131072], P('ta', None, None, None, ('px', 'py'))
- gram: float32 [32, 2, 2, 2], P('ta')
The draws below stay inside these ranges and needn't reach their ends.
All inputs are finite; a program needn't handle non-finite values.
Results may differ from the reference program's by a relative error of at most 0.0042.
Values may be sent and summed in bfloat16 or wider, within the bound.
A program may use at most 128 MiB of HBM per device.

```python
import math
import jax
import jax.numpy as jnp
from jax import lax

VARS = 5
BLK = 256
HOP = 128
SEGMENT_NUMBER = 2
RECORD_LENGTH = 384
RETAINED_MODES = 32
POINTS = 131072


def place_ends(values, key, least, high):
    index_at = [jax.random.randint(jax.random.fold_in(key, axis), (), 0, length) for axis, length in enumerate(values.shape)]
    widest = values.shape.index(max(values.shape))
    beside = index_at[:widest] + [(index_at[widest] + 1) % values.shape[widest]] + index_at[widest + 1:]
    return values.at[tuple(index_at)].set(least).at[tuple(beside)].set(high)


def block_levels(key, dims, cuts, low, top_value):
    def one(axis_at, parts):
        draws = jax.random.uniform(jax.random.fold_in(jax.random.fold_in(key, 6), axis_at), (parts,), jnp.float32, low / len(cuts), top_value / len(cuts))
        return jnp.repeat(jnp.exp(draws), dims[axis_at] // parts).reshape((-1,) + (1,) * (len(dims) - axis_at - 1))

    loudness = one(*cuts[0])
    for cut in cuts[1:]:
        loudness = loudness * one(*cut)
    return loudness


def scatter_about(rng, dims, spread, most, pieces=(), kind=jnp.bfloat16):
    loudness = block_levels(rng, dims, pieces, -0.22, 0.18) if pieces else 1.0
    entries = jax.random.normal(rng, dims, jnp.float32) * spread * loudness
    return jnp.minimum(jnp.maximum(entries, -most), most).astype(kind)


def setup_inputs(seed: int = 0) -> dict:
    key_list = jax.random.split(jax.random.key(seed), 4)
    return {
        "snapshots": scatter_about(key_list[0], (RECORD_LENGTH, VARS, POINTS), 1.0, 6.0, ((0, 16), (2, 16))),
        "quad_weights": jnp.clip(jnp.exp(math.log(10.0) - 2.3025851 * jax.random.uniform(key_list[1], (POINTS,), jnp.float32) ** block_levels(key_list[1], (POINTS,), ((0, 16),), -0.2, 0.2)), 1.0, 10.0),
        "spectral_indices": place_ends(jax.random.randint(key_list[2], (RETAINED_MODES,), 0, BLK // 2), jax.random.fold_in(key_list[2], 1), 0, (BLK // 2) - 1).astype(jnp.int32),
    }


def make_rotation_multipliers(spectral_indices, temporal_locations):
    segment_beginnings = jnp.arange(SEGMENT_NUMBER, dtype=jnp.int32) * HOP
    segment_shifts = temporal_locations[None, :] - segment_beginnings[:, None]
    inside = (segment_shifts >= 0) & (segment_shifts < BLK)
    window = 0.5 - 0.5 * jnp.cos(2.0 * math.pi * segment_shifts.astype(jnp.float32) / BLK)
    window = jnp.where(inside, window, jnp.float32(0.0)) / jnp.sqrt(jnp.float32(3.0 * BLK / 8.0))
    phases = jnp.mod(spectral_indices[:, None, None] * segment_shifts[None, :, :], BLK)
    angles = 2.0 * math.pi * phases.astype(jnp.float32) / BLK
    real_part = jnp.cos(angles) * window[None]
    imag_part = -jnp.sin(angles) * window[None]
    gathered_segments = jnp.stack([real_part, imag_part], axis=2)
    return gathered_segments.reshape(RETAINED_MODES * SEGMENT_NUMBER * 2, temporal_locations.shape[0]).astype(jnp.bfloat16)

def gram_terms(spectra):
    flat = spectra.reshape(spectra.shape[0], 2 * SEGMENT_NUMBER, -1)
    inner = jnp.einsum('fam,fbm->fab', flat, flat, precision=lax.Precision.HIGHEST)
    inner = inner.reshape(spectra.shape[0], SEGMENT_NUMBER, 2, SEGMENT_NUMBER, 2)
    real_part = inner[:, :, 0, :, 0] + inner[:, :, 1, :, 1]
    imag_part = inner[:, :, 0, :, 1] - inner[:, :, 1, :, 0]
    return jnp.stack([real_part, imag_part], axis=-1)

def reference(snapshots, quad_weights, spectral_indices):
    temporal_locations = jnp.arange(RECORD_LENGTH, dtype=jnp.int32)
    rotation_multipliers = make_rotation_multipliers(spectral_indices, temporal_locations)
    flat_snapshots = snapshots.reshape(RECORD_LENGTH, VARS * POINTS)
    raw = jnp.dot(rotation_multipliers, flat_snapshots, preferred_element_type=jnp.float32)
    raw = raw.reshape(RETAINED_MODES, SEGMENT_NUMBER, 2, VARS, POINTS)
    spectra = raw * jnp.sqrt(quad_weights)
    gram = gram_terms(spectra) / jnp.float32(POINTS * VARS)
    return (spectra, gram)
```

```python
import functools
import math

import jax
import jax.numpy as jnp
from jax import lax
from jax.experimental import pallas as pl
from jax.experimental.pallas import tpu as pltpu
from jax.sharding import PartitionSpec as P

VARS = 5
BLK = 256
HOP = 128
SEGMENT_NUMBER = 2
RECORD_LENGTH = 384
RETAINED_MODES = 32
ROWS = RETAINED_MODES * SEGMENT_NUMBER * 2
MESH = pl.DeviceIdType.MESH
LANES = 128
STEPS = (
    (0, 1), (0, 3), (1, 0), (3, 0), (0, 2), (2, 0), (1, 1), (3, 3),
    (1, 3), (3, 1), (2, 1), (2, 3), (1, 2), (3, 2), (2, 2),
)


def cosine(phase):
    k = jnp.bitwise_and(phase, BLK - 1)
    k = jnp.where(k > BLK // 2, BLK - k, k)
    far = k > BLK // 4
    k = jnp.where(far, BLK // 2 - k, k)
    a = k.astype(jnp.float32) * jnp.float32(2.0 * math.pi / BLK)
    s = a * a
    total = jnp.float32(1.0 / math.factorial(12))
    for n in (10, 8, 6, 4, 2, 0):
        total = total * s * -1.0 if n == 10 else total * s
        total = total + jnp.float32((-1.0) ** (n // 2) / math.factorial(n))
    return jnp.where(far, -total, total)


def exchange_kernel(
    groups, width, cores, depth,
    snap, weights, indices, out, gram_out,
    mine, arrived, twiddles, terms, staged, w_ref, idx_ref, squares, crosses, gram_mine, gram_seen, gram_sum,
    load_sem, own_sem, small_sem, send_sem, recv_sem, send_two, recv_two, gram_send, gram_recv, last_send, last_recv,
):
    me = lax.axis_index("ta")
    px, py = lax.axis_index("px"), lax.axis_index("py")
    side = math.isqrt(groups)
    y, x = me // side, me % side
    peers = [lax.rem(y + dy, side) * side + lax.rem(x + dx, side) for dy, dx in STEPS]
    place = px * depth + py
    others = [(dp, dz) for dz in range(depth) for dp in range(cores) if (dp, dz) != (0, 0)]
    planes = [(lax.rem(px + dp, cores), lax.rem(py + dz, depth)) for dp, dz in others]

    index_copy = pltpu.make_async_copy(indices, idx_ref, small_sem.at[0])
    index_copy.start()
    weight_copy = pltpu.make_async_copy(weights, w_ref, small_sem.at[1])
    weight_copy.start()
    loads = [pltpu.make_async_copy(snap.at[v], mine.at[v], load_sem.at[v]) for v in range(VARS)]
    for load in loads:
        load.start()
    own = pl.ds(pl.multiple_of(me * width, LANES), width)
    for v in range(VARS):
        pltpu.make_async_copy(snap.at[v, :, own], arrived.at[v, me], own_sem.at[v]).start()

    barrier = pltpu.get_barrier_semaphore()
    for peer in peers:
        pl.semaphore_signal(barrier, inc=1, device_id={"ta": peer}, device_id_type=MESH)
    for p, z in planes:
        pl.semaphore_signal(barrier, inc=1, device_id={"px": p, "py": z}, device_id_type=MESH)

    index_copy.wait()
    shape = (8, RECORD_LENGTH)
    row = lax.broadcasted_iota(jnp.int32, shape, 0)
    lag = lax.broadcasted_iota(jnp.int32, shape, 1) - HOP * jnp.bitwise_and(row // 2, 1)
    turn = (BLK // 4) * jnp.bitwise_and(row, 1)
    inside = (lag >= 0) & (lag < BLK)
    window = jnp.float32(0.5) - jnp.float32(0.5) * cosine(lag)
    window = jnp.where(inside, window, jnp.float32(0.0)) / jnp.sqrt(jnp.float32(3.0 * BLK / 8.0))

    def fill(g, carry):
        index = jnp.where(row < 4, idx_ref[2 * g], idx_ref[2 * g + 1])
        rows = pl.ds(pl.multiple_of(g * 8, 8), 8)
        twiddles[rows, :] = cosine(index * lag + turn) * window
        squares[rows, :] = jnp.zeros((8, LANES), jnp.float32)
        crosses[rows, :] = jnp.zeros((8, LANES), jnp.float32)
        return carry

    lax.fori_loop(0, ROWS // 8, fill, 0)
    weight_copy.wait()
    for load in loads:
        load.wait()
    pl.semaphore_wait(barrier, len(peers) + len(planes))

    def to_owner(v, peer):
        cut = pl.ds(pl.multiple_of(peer * width, LANES), width)
        return pltpu.make_async_remote_copy(
            src_ref=mine.at[v, :, cut], dst_ref=arrived.at[v, me], send_sem=send_sem.at[v], recv_sem=recv_sem.at[v],
            device_id={"ta": peer}, device_id_type=MESH,
        )

    def send_all(v, carry):
        for peer in peers:
            to_owner(v, peer).start()
        return carry

    lax.fori_loop(0, VARS, send_all, 0)
    line = lax.broadcasted_iota(jnp.int32, (8, LANES), 0)
    quarter = jnp.bitwise_and(line, 3)

    def work(v, carry):
        pltpu.make_async_copy(arrived.at[v, pl.ds(0, groups - 1)], arrived.at[v, pl.ds(0, groups - 1)], recv_sem.at[v]).wait()
        pltpu.make_async_copy(snap.at[v, :, own], arrived.at[v, me], own_sem.at[v]).wait()
        series = arrived[v].reshape(RECORD_LENGTH, width)
        raw = jnp.dot(twiddles[...].astype(jnp.bfloat16), series, preferred_element_type=jnp.float32)
        terms[...] = raw
        staged[v] = raw.astype(jnp.bfloat16).reshape(groups, 8, width)

        def gather(g, inner):
            rows = pl.ds(pl.multiple_of(g * 8, 8), 8)
            square = squares[rows, :]
            cross = crosses[rows, :]
            for j in range(width // LANES):
                a = terms[rows, j * LANES : (j + 1) * LANES]
                w = w_ref[pl.ds(me * (width // LANES) + j, 1), :]
                first = jnp.where(quarter < 2, a, pltpu.roll(a, 2, 0))
                second = jnp.where(quarter < 2, pltpu.roll(a, 6, 0), jnp.where(quarter == 2, pltpu.roll(a, 7, 0), pltpu.roll(a, 1, 0)))
                square = square + a * a * w
                cross = cross + first * second * w
            squares[rows, :] = square
            crosses[rows, :] = cross
            return inner

        lax.fori_loop(0, ROWS // 8, gather, 0)
        for peer in peers:
            pltpu.make_async_remote_copy(
                src_ref=staged.at[v, peer], dst_ref=out.at[v, me], send_sem=send_two.at[v], recv_sem=recv_two.at[v],
                device_id={"ta": peer}, device_id_type=MESH,
            ).start()
        out[v, me] = staged[v, me]
        return carry

    lax.fori_loop(0, VARS, work, 0)

    diagonal = lax.broadcasted_iota(jnp.int32, (ROWS, LANES), 0) == lax.broadcasted_iota(jnp.int32, (ROWS, LANES), 1)

    def in_lanes(ref):
        sums = jnp.sum(ref[...], axis=1, keepdims=True)
        return jnp.sum(jnp.where(diagonal, sums, jnp.float32(0.0)), axis=0, keepdims=True)

    both = jnp.where(line == 0, in_lanes(squares), in_lanes(crosses))
    gram_mine[...] = both
    gram_seen[place] = both
    for i, (p, z) in enumerate(planes):
        pltpu.make_async_remote_copy(
            src_ref=gram_mine, dst_ref=gram_seen.at[place], send_sem=gram_send, recv_sem=gram_recv,
            device_id={"px": p, "py": z}, device_id_type=MESH,
        ).start()
    n_planes = len(planes)
    pltpu.make_async_copy(gram_seen.at[pl.ds(0, n_planes)], gram_seen.at[pl.ds(0, n_planes)], gram_recv).wait()
    whole = jnp.sum(gram_seen[...], axis=0)
    gram_sum[...] = whole
    gram_out[me] = whole
    for peer in peers:
        pltpu.make_async_remote_copy(
            src_ref=gram_sum, dst_ref=gram_out.at[me], send_sem=last_send, recv_sem=last_recv,
            device_id={"ta": peer}, device_id_type=MESH,
        ).start()

    n = len(peers)
    for v in range(VARS):
        pltpu.make_async_copy(out.at[v, pl.ds(0, n)], out.at[v, pl.ds(0, n)], recv_two.at[v]).wait()
    pltpu.make_async_copy(gram_out.at[pl.ds(0, n)], gram_out.at[pl.ds(0, n)], last_recv).wait()
    for v in range(VARS):
        pltpu.make_async_copy(arrived.at[v, pl.ds(0, n)], arrived.at[v, pl.ds(0, n)], send_sem.at[v]).wait()
        pltpu.make_async_copy(out.at[v, pl.ds(0, n)], out.at[v, pl.ds(0, n)], send_two.at[v]).wait()
    pltpu.make_async_copy(gram_seen.at[pl.ds(0, n_planes)], gram_seen.at[pl.ds(0, n_planes)], gram_send).wait()
    pltpu.make_async_copy(gram_out.at[pl.ds(0, n)], gram_out.at[pl.ds(0, n)], last_send).wait()


def finish_kernel(groups, width, total, held, w_ref, gram_in, out, gram):
    def scale(k, carry):
        lanes = pl.ds(pl.multiple_of(k * width, LANES), width)
        for j in range(width // LANES):
            root = jnp.sqrt(w_ref[pl.ds(k * (width // LANES) + j, 1), :])
            part = held[0, k, :, j * LANES : (j + 1) * LANES].astype(jnp.float32) * root
            at = pl.ds(pl.multiple_of(k * width + j * LANES, LANES), LANES)
            for i in range(4):
                out[i, 0, :, at] = part[2 * i : 2 * i + 2, :]
        return carry

    lax.fori_loop(0, groups, scale, 0)

    @pl.when(pl.program_id(0) == 0)
    def _():
        me = lax.axis_index("ta")
        sums = jnp.sum(gram_in[...], axis=0) / jnp.float32(total)
        sums = pltpu.roll(sums, lax.rem(LANES - 8 * me, LANES), 1)
        r = lax.broadcasted_iota(jnp.int32, (2, 2), 0)
        c = lax.broadcasted_iota(jnp.int32, (2, 2), 1)

        def entry(kind, lane):
            return jnp.broadcast_to(sums[kind : kind + 1, lane : lane + 1], (2, 2))

        zero = jnp.zeros((2, 2), jnp.float32)
        for f in range(2):
            real = entry(1, 4 * f) + entry(1, 4 * f + 1)
            imag = entry(1, 4 * f + 2) - entry(1, 4 * f + 3)
            for b in range(2):
                power = entry(0, 4 * f + 2 * b) + entry(0, 4 * f + 2 * b + 1)
                crossed = jnp.where(c == 0, real, imag if b == 0 else -imag)
                gram[f, b] = jnp.where(r == b, jnp.where(c == 0, power, zero), crossed)


def solution(mesh):
    groups, cores, depth = mesh.shape["ta"], mesh.shape["px"], mesh.shape["py"]

    def on_device(snapshots, quad_weights, spectral_indices):
        steps, _, points = snapshots.shape
        width = points // groups
        series = jnp.transpose(snapshots, (1, 0, 2))
        weights = quad_weights.reshape(points // LANES, LANES)
        anywhere = pl.BlockSpec(memory_space=pl.ANY)
        vmem = pl.BlockSpec(memory_space=pltpu.VMEM)
        held, gram_parts = pl.pallas_call(
            functools.partial(exchange_kernel, groups, width, cores, depth),
            name="exchange",
            out_shape=(
                jax.ShapeDtypeStruct((VARS, groups, 8, width), jnp.bfloat16),
                jax.ShapeDtypeStruct((groups, 8, LANES), jnp.float32),
            ),
            in_specs=[anywhere, anywhere, anywhere],
            out_specs=(vmem, vmem),
            scratch_shapes=[
                pltpu.VMEM((VARS, steps, points), jnp.bfloat16),
                pltpu.VMEM((VARS, groups, steps, width), jnp.bfloat16),
                pltpu.VMEM((ROWS, RECORD_LENGTH), jnp.float32),
                pltpu.VMEM((ROWS, width), jnp.float32),
                pltpu.VMEM((VARS, groups, 8, width), jnp.bfloat16),
                pltpu.VMEM((points // LANES, LANES), jnp.float32),
                pltpu.SMEM((RETAINED_MODES,), jnp.int32),
                pltpu.VMEM((ROWS, LANES), jnp.float32),
                pltpu.VMEM((ROWS, LANES), jnp.float32),
                pltpu.VMEM((8, LANES), jnp.float32),
                pltpu.VMEM((cores * depth, 8, LANES), jnp.float32),
                pltpu.VMEM((8, LANES), jnp.float32),
                pltpu.SemaphoreType.DMA((VARS,)),
                pltpu.SemaphoreType.DMA((VARS,)),
                pltpu.SemaphoreType.DMA((2,)),
                pltpu.SemaphoreType.DMA((VARS,)),
                pltpu.SemaphoreType.DMA((VARS,)),
                pltpu.SemaphoreType.DMA((VARS,)),
                pltpu.SemaphoreType.DMA((VARS,)),
                pltpu.SemaphoreType.DMA,
                pltpu.SemaphoreType.DMA,
                pltpu.SemaphoreType.DMA,
                pltpu.SemaphoreType.DMA,
            ],
            compiler_params=pltpu.CompilerParams(collective_id=0, has_side_effects=True, vmem_limit_bytes=32 * 2**20),
        )(series, weights, spectral_indices)
        total = points * cores * depth * VARS
        spectra, gram = pl.pallas_call(
            functools.partial(finish_kernel, groups, width, total),
            name="finish",
            grid=(VARS,),
            out_shape=(
                jax.ShapeDtypeStruct((4, VARS, 2, points), jnp.float32),
                jax.ShapeDtypeStruct((2, 2, 2, 2), jnp.float32),
            ),
            in_specs=[pl.BlockSpec((1, groups, 8, width), lambda v: (v, 0, 0, 0)), vmem, vmem],
            out_specs=(
                pl.BlockSpec((4, 1, 2, points), lambda v: (0, v, 0, 0)),
                vmem,
            ),
        )(held, weights, gram_parts)
        spectra = spectra.reshape(2, SEGMENT_NUMBER, VARS, 2, points).transpose(0, 1, 3, 2, 4)
        return (spectra, gram)

    return jax.shard_map(
        on_device,
        mesh=mesh,
        in_specs=(P("ta", None, ("px", "py")), P(("px", "py")), P()),
        out_specs=(P("ta", None, None, None, ("px", "py")), P("ta", None, None, None)),
        check_vma=False,
    )
```

```python
import functools
import math

import jax
import jax.numpy as jnp
from jax import lax
from jax.experimental import pallas as pl
from jax.experimental.pallas import tpu as pltpu
from jax.sharding import PartitionSpec as P

VARS = 5
BLK = 256
HOP = 128
SEGMENT_NUMBER = 2
RECORD_LENGTH = 384
RETAINED_MODES = 32
ROWS = RETAINED_MODES * SEGMENT_NUMBER * 2
MESH = pl.DeviceIdType.MESH
LANES = 128
STEPS = (
    (0, 1), (0, 3), (1, 0), (3, 0), (0, 2), (2, 0), (1, 1), (3, 3),
    (1, 3), (3, 1), (2, 1), (2, 3), (1, 2), (3, 2), (2, 2),
)


def cosine(phase):
    k = jnp.bitwise_and(phase, BLK - 1)
    k = jnp.where(k > BLK // 2, BLK - k, k)
    far = k > BLK // 4
    k = jnp.where(far, BLK // 2 - k, k)
    a = k.astype(jnp.float32) * jnp.float32(2.0 * math.pi / BLK)
    s = a * a
    total = jnp.float32(1.0 / math.factorial(12))
    for n in (10, 8, 6, 4, 2, 0):
        total = total * s * -1.0 if n == 10 else total * s
        total = total + jnp.float32((-1.0) ** (n // 2) / math.factorial(n))
    return jnp.where(far, -total, total)


def exchange_kernel(
    groups, width, cores, depth,
    snap, weights, indices, spectra, gram_out,
    mine, arrived, twiddles, terms, staged, out, w_ref, roots, idx_ref, squares, crosses, gram_mine, gram_seen, gram_sum,
    load_sem, own_sem, small_sem, send_sem, recv_sem, send_two, recv_two, gram_send, gram_recv, last_send, last_recv,
):
    me = lax.axis_index("ta")
    px, py = lax.axis_index("px"), lax.axis_index("py")
    side = math.isqrt(groups)
    y, x = me // side, me % side
    peers = [lax.rem(y + dy, side) * side + lax.rem(x + dx, side) for dy, dx in STEPS]
    place = px * depth + py
    others = [(dp, dz) for dz in range(depth) for dp in range(cores) if (dp, dz) != (0, 0)]
    planes = [(lax.rem(px + dp, cores), lax.rem(py + dz, depth)) for dp, dz in others]

    index_copy = pltpu.make_async_copy(indices, idx_ref, small_sem.at[0])
    index_copy.start()
    weight_copy = pltpu.make_async_copy(weights, w_ref, small_sem.at[1])
    weight_copy.start()
    loads = [pltpu.make_async_copy(snap.at[v], mine.at[v], load_sem.at[v]) for v in range(VARS)]
    for load in loads:
        load.start()
    own = pl.ds(pl.multiple_of(me * width, LANES), width)
    for v in range(VARS):
        pltpu.make_async_copy(snap.at[v, :, own], arrived.at[v, me], own_sem.at[v]).start()

    barrier = pltpu.get_barrier_semaphore()
    for peer in peers:
        pl.semaphore_signal(barrier, inc=1, device_id={"ta": peer}, device_id_type=MESH)
    for p, z in planes:
        pl.semaphore_signal(barrier, inc=1, device_id={"px": p, "py": z}, device_id_type=MESH)

    index_copy.wait()
    shape = (8, RECORD_LENGTH)
    row = lax.broadcasted_iota(jnp.int32, shape, 0)
    lag = lax.broadcasted_iota(jnp.int32, shape, 1) - HOP * jnp.bitwise_and(row // 2, 1)
    turn = (BLK // 4) * jnp.bitwise_and(row, 1)
    inside = (lag >= 0) & (lag < BLK)
    window = jnp.float32(0.5) - jnp.float32(0.5) * cosine(lag)
    window = jnp.where(inside, window, jnp.float32(0.0)) / jnp.sqrt(jnp.float32(3.0 * BLK / 8.0))

    def fill(g, carry):
        index = jnp.where(row < 4, idx_ref[2 * g], idx_ref[2 * g + 1])
        rows = pl.ds(pl.multiple_of(g * 8, 8), 8)
        twiddles[rows, :] = cosine(index * lag + turn) * window
        squares[rows, :] = jnp.zeros((8, LANES), jnp.float32)
        crosses[rows, :] = jnp.zeros((8, LANES), jnp.float32)
        return carry

    lax.fori_loop(0, ROWS // 8, fill, 0)
    weight_copy.wait()
    for load in loads:
        load.wait()
    pl.semaphore_wait(barrier, len(peers) + len(planes))

    def to_owner(v, peer):
        cut = pl.ds(pl.multiple_of(peer * width, LANES), width)
        return pltpu.make_async_remote_copy(
            src_ref=mine.at[v, :, cut], dst_ref=arrived.at[v, me], send_sem=send_sem.at[v], recv_sem=recv_sem.at[v],
            device_id={"ta": peer}, device_id_type=MESH,
        )

    def send_all(v, carry):
        for peer in peers:
            to_owner(v, peer).start()
        return carry

    lax.fori_loop(0, VARS, send_all, 0)
    line = lax.broadcasted_iota(jnp.int32, (8, LANES), 0)
    quarter = jnp.bitwise_and(line, 3)

    def work(v, carry):
        pltpu.make_async_copy(arrived.at[v, pl.ds(0, groups - 1)], arrived.at[v, pl.ds(0, groups - 1)], recv_sem.at[v]).wait()
        pltpu.make_async_copy(snap.at[v, :, own], arrived.at[v, me], own_sem.at[v]).wait()
        series = arrived[v].reshape(RECORD_LENGTH, width)
        raw = jnp.dot(twiddles[...].astype(jnp.bfloat16), series, preferred_element_type=jnp.float32)
        terms[...] = raw
        staged[v] = raw.astype(jnp.bfloat16).reshape(groups, 8, width)

        def gather(g, inner):
            rows = pl.ds(pl.multiple_of(g * 8, 8), 8)
            square = squares[rows, :]
            cross = crosses[rows, :]
            for j in range(width // LANES):
                a = terms[rows, j * LANES : (j + 1) * LANES]
                w = w_ref[pl.ds(me * (width // LANES) + j, 1), :]
                first = jnp.where(quarter < 2, a, pltpu.roll(a, 2, 0))
                second = jnp.where(quarter < 2, pltpu.roll(a, 6, 0), jnp.where(quarter == 2, pltpu.roll(a, 7, 0), pltpu.roll(a, 1, 0)))
                square = square + a * a * w
                cross = cross + first * second * w
            squares[rows, :] = square
            crosses[rows, :] = cross
            return inner

        lax.fori_loop(0, ROWS // 8, gather, 0)
        for peer in peers:
            pltpu.make_async_remote_copy(
                src_ref=staged.at[v, peer], dst_ref=out.at[v, me], send_sem=send_two.at[v], recv_sem=recv_two.at[v],
                device_id={"ta": peer}, device_id_type=MESH,
            ).start()
        out[v, me] = staged[v, me]
        return carry

    lax.fori_loop(0, VARS, work, 0)

    diagonal = lax.broadcasted_iota(jnp.int32, (ROWS, LANES), 0) == lax.broadcasted_iota(jnp.int32, (ROWS, LANES), 1)

    def in_lanes(ref):
        sums = jnp.sum(ref[...], axis=1, keepdims=True)
        return jnp.sum(jnp.where(diagonal, sums, jnp.float32(0.0)), axis=0, keepdims=True)

    both = jnp.where(line == 0, in_lanes(squares), in_lanes(crosses))
    gram_mine[...] = both
    gram_seen[place] = both
    for i, (p, z) in enumerate(planes):
        pltpu.make_async_remote_copy(
            src_ref=gram_mine, dst_ref=gram_seen.at[place], send_sem=gram_send, recv_sem=gram_recv,
            device_id={"px": p, "py": z}, device_id_type=MESH,
        ).start()
    n_planes = len(planes)
    pltpu.make_async_copy(gram_seen.at[pl.ds(0, n_planes)], gram_seen.at[pl.ds(0, n_planes)], gram_recv).wait()
    whole = jnp.sum(gram_seen[...], axis=0)
    gram_sum[...] = whole
    gram_out[me] = whole
    for peer in peers:
        pltpu.make_async_remote_copy(
            src_ref=gram_sum, dst_ref=gram_out.at[me], send_sem=last_send, recv_sem=last_recv,
            device_id={"ta": peer}, device_id_type=MESH,
        ).start()

    n = len(peers)
    tiles = width // LANES
    roots[...] = jnp.sqrt(w_ref[...])

    def scale(v, carry):
        pltpu.make_async_copy(out.at[v, pl.ds(0, n)], out.at[v, pl.ds(0, n)], recv_two.at[v]).wait()

        def one(k, inner):
            for j in range(tiles):
                root = roots[pl.ds(k * tiles + j, 1), :]
                part = out[v, k, :, j * LANES : (j + 1) * LANES].astype(jnp.float32) * root
                at = pl.ds(pl.multiple_of(k * width + j * LANES, LANES), LANES)
                for i in range(4):
                    spectra[i, v, :, at] = part[2 * i : 2 * i + 2, :]
            return inner

        lax.fori_loop(0, groups, one, 0)
        return carry

    lax.fori_loop(0, VARS, scale, 0)
    pltpu.make_async_copy(gram_out.at[pl.ds(0, n)], gram_out.at[pl.ds(0, n)], last_recv).wait()
    for v in range(VARS):
        pltpu.make_async_copy(arrived.at[v, pl.ds(0, n)], arrived.at[v, pl.ds(0, n)], send_sem.at[v]).wait()
        pltpu.make_async_copy(out.at[v, pl.ds(0, n)], out.at[v, pl.ds(0, n)], send_two.at[v]).wait()
    pltpu.make_async_copy(gram_seen.at[pl.ds(0, n_planes)], gram_seen.at[pl.ds(0, n_planes)], gram_send).wait()
    pltpu.make_async_copy(gram_out.at[pl.ds(0, n)], gram_out.at[pl.ds(0, n)], last_send).wait()


def finish_kernel(total, spectra, gram_in, out, gram, sem):
    copies = [pltpu.make_async_copy(spectra.at[i], out.at[i], sem.at[i]) for i in range(4)]
    for copy in copies:
        copy.start()
    me = lax.axis_index("ta")
    sums = jnp.sum(gram_in[...], axis=0) / jnp.float32(total)
    sums = pltpu.roll(sums, lax.rem(LANES - 8 * me, LANES), 1)
    r = lax.broadcasted_iota(jnp.int32, (2, 2), 0)
    c = lax.broadcasted_iota(jnp.int32, (2, 2), 1)

    def entry(kind, lane):
        return jnp.broadcast_to(sums[kind : kind + 1, lane : lane + 1], (2, 2))

    zero = jnp.zeros((2, 2), jnp.float32)
    for f in range(2):
        real = entry(1, 4 * f) + entry(1, 4 * f + 1)
        imag = entry(1, 4 * f + 2) - entry(1, 4 * f + 3)
        for b in range(2):
            power = entry(0, 4 * f + 2 * b) + entry(0, 4 * f + 2 * b + 1)
            crossed = jnp.where(c == 0, real, imag if b == 0 else -imag)
            gram[f, b] = jnp.where(r == b, jnp.where(c == 0, power, zero), crossed)
    for copy in copies:
        copy.wait()


def solution(mesh):
    groups, cores, depth = mesh.shape["ta"], mesh.shape["px"], mesh.shape["py"]

    def on_device(snapshots, quad_weights, spectral_indices):
        steps, _, points = snapshots.shape
        width = points // groups
        series = jnp.transpose(snapshots, (1, 0, 2))
        weights = quad_weights.reshape(points // LANES, LANES)
        hbm = pl.BlockSpec(memory_space=pltpu.HBM)
        vmem = pl.BlockSpec(memory_space=pltpu.VMEM)
        spectra, gram_parts = pl.pallas_call(
            functools.partial(exchange_kernel, groups, width, cores, depth),
            name="exchange",
            out_shape=(
                jax.ShapeDtypeStruct((4, VARS, 2, points), jnp.float32),
                jax.ShapeDtypeStruct((groups, 8, LANES), jnp.float32),
            ),
            in_specs=[hbm, hbm, hbm],
            out_specs=(vmem, vmem),
            scratch_shapes=[
                pltpu.VMEM((VARS, steps, points), jnp.bfloat16),
                pltpu.VMEM((VARS, groups, steps, width), jnp.bfloat16),
                pltpu.VMEM((ROWS, RECORD_LENGTH), jnp.float32),
                pltpu.VMEM((ROWS, width), jnp.float32),
                pltpu.VMEM((VARS, groups, 8, width), jnp.bfloat16),
                pltpu.VMEM((VARS, groups, 8, width), jnp.bfloat16),
                pltpu.VMEM((points // LANES, LANES), jnp.float32),
                pltpu.VMEM((points // LANES, LANES), jnp.float32),
                pltpu.SMEM((RETAINED_MODES,), jnp.int32),
                pltpu.VMEM((ROWS, LANES), jnp.float32),
                pltpu.VMEM((ROWS, LANES), jnp.float32),
                pltpu.VMEM((8, LANES), jnp.float32),
                pltpu.VMEM((cores * depth, 8, LANES), jnp.float32),
                pltpu.VMEM((8, LANES), jnp.float32),
                pltpu.SemaphoreType.DMA((VARS,)),
                pltpu.SemaphoreType.DMA((VARS,)),
                pltpu.SemaphoreType.DMA((2,)),
                pltpu.SemaphoreType.DMA((VARS,)),
                pltpu.SemaphoreType.DMA((VARS,)),
                pltpu.SemaphoreType.DMA((VARS,)),
                pltpu.SemaphoreType.DMA((VARS,)),
                pltpu.SemaphoreType.DMA,
                pltpu.SemaphoreType.DMA,
                pltpu.SemaphoreType.DMA,
                pltpu.SemaphoreType.DMA,
            ],
            compiler_params=pltpu.CompilerParams(collective_id=0, has_side_effects=True, vmem_limit_bytes=32 * 2**20),
        )(*(pltpu.with_memory_space_constraint(a, pltpu.HBM) for a in (series, weights, spectral_indices)))
        total = points * cores * depth * VARS
        spectra, gram = pl.pallas_call(
            functools.partial(finish_kernel, total),
            name="finish",
            out_shape=(
                jax.ShapeDtypeStruct((4, VARS, 2, points), jnp.float32),
                jax.ShapeDtypeStruct((2, 2, 2, 2), jnp.float32),
            ),
            in_specs=[vmem, vmem],
            out_specs=(hbm, vmem),
            scratch_shapes=[pltpu.SemaphoreType.DMA((4,))],
            compiler_params=pltpu.CompilerParams(vmem_limit_bytes=8 * 2**20),
        )(spectra, gram_parts)
        spectra = spectra.reshape(2, SEGMENT_NUMBER, VARS, 2, points).transpose(0, 1, 3, 2, 4)
        return (spectra, gram)

    return jax.shard_map(
        on_device,
        mesh=mesh,
        in_specs=(P("ta", None, ("px", "py")), P(("px", "py")), P()),
        out_specs=(P("ta", None, None, None, ("px", "py")), P("ta", None, None, None)),
        check_vma=False,
    )
```

```python
import functools
import math

import jax
import jax.numpy as jnp
from jax import lax
from jax.experimental import pallas as pl
from jax.experimental.pallas import tpu as pltpu
from jax.sharding import PartitionSpec as P

VARS = 5
BLK = 256
HOP = 128
SEGMENT_NUMBER = 2
RECORD_LENGTH = 384
RETAINED_MODES = 32
ROWS = RETAINED_MODES * SEGMENT_NUMBER * 2
MESH = pl.DeviceIdType.MESH
LANES = 128
STEPS = (
    (0, 1), (0, 3), (1, 0), (3, 0), (0, 2), (2, 0), (1, 1), (3, 3),
    (1, 3), (3, 1), (2, 1), (2, 3), (1, 2), (3, 2), (2, 2),
)
NEAR, SECOND, THIRD = slice(0, 4), slice(4, 10), slice(10, 14)


def cosine(phase):
    k = jnp.bitwise_and(phase, BLK - 1)
    k = jnp.where(k > BLK // 2, BLK - k, k)
    far = k > BLK // 4
    k = jnp.where(far, BLK // 2 - k, k)
    a = k.astype(jnp.float32) * jnp.float32(2.0 * math.pi / BLK)
    s = a * a
    total = jnp.float32(1.0 / math.factorial(12))
    for n in (10, 8, 6, 4, 2, 0):
        total = total * s * -1.0 if n == 10 else total * s
        total = total + jnp.float32((-1.0) ** (n // 2) / math.factorial(n))
    return jnp.where(far, -total, total)


def exchange_kernel(
    groups, width, cores, depth,
    snap, weights, indices, spectra, gram_out,
    mine, arrived, multipliers, twiddles, terms, turned, staged, held, w_ref, roots, idx_ref, sums, gram_mine, gram_seen, gram_sum,
    load_sem, own_sem, small_sem, send_sem, recv_sem, send_two, recv_two, gram_send, gram_recv, last_send, last_recv, known, here, everyone,
):
    me = lax.axis_index("ta")
    px, py = lax.axis_index("px"), lax.axis_index("py")
    side = math.isqrt(groups)
    y, x = me // side, me % side
    peers = [lax.rem(y + dy, side) * side + lax.rem(x + dx, side) for dy, dx in STEPS]
    place = px * depth + py
    others = [(dp, dz) for dz in range(depth) for dp in range(cores) if (dp, dz) != (0, 0)]
    planes = [(lax.rem(px + dp, cores), lax.rem(py + dz, depth)) for dp, dz in others]
    n, n_planes, tiles = len(peers), len(planes), width // LANES

    index_copy = pltpu.make_async_copy(indices, idx_ref, small_sem.at[0])
    index_copy.start()
    weight_copy = pltpu.make_async_copy(weights, w_ref, small_sem.at[1])
    weight_copy.start()
    loads = [pltpu.make_async_copy(snap.at[v], mine.at[v], load_sem.at[v]) for v in range(VARS)]
    for load in loads:
        load.start()
    own = pl.ds(pl.multiple_of(me * width, LANES), width)
    for v in range(VARS):
        pltpu.make_async_copy(snap.at[v, :, own], arrived.at[v, me], own_sem.at[v]).start()

    barrier = pltpu.get_barrier_semaphore()
    for peer in peers[NEAR]:
        pl.semaphore_signal(barrier, inc=1, device_id={"ta": peer}, device_id_type=MESH)

    @pl.when(place == 0)
    def _():
        for p, z in planes:
            pl.semaphore_signal(barrier, inc=1, device_id={"px": p, "py": z}, device_id_type=MESH)

    pl.semaphore_wait(barrier, jnp.where(place == 0, 4, 5))

    def tell(i):
        for peer in peers[NEAR]:
            pl.semaphore_signal(known.at[i], inc=1, device_id={"ta": peer}, device_id_type=MESH)

    def send(v, to):
        for peer in to:
            cut = pl.ds(pl.multiple_of(peer * width, LANES), width)
            pltpu.make_async_remote_copy(
                src_ref=mine.at[v, :, cut], dst_ref=arrived.at[v, me], send_sem=send_sem.at[v], recv_sem=recv_sem.at[v],
                device_id={"ta": peer}, device_id_type=MESH,
            ).start()

    def send_each(to):
        def step(v, carry):
            send(v, to)
            return carry

        return step

    tell(0)

    @pl.when(place != 0)
    def _():
        pl.semaphore_signal(here, inc=1, device_id={"px": 0, "py": 0}, device_id_type=MESH)

    for load in loads:
        load.wait()
    lax.fori_loop(0, VARS, send_each(peers[NEAR]), 0)
    pl.semaphore_wait(known.at[0], 4)
    tell(1)
    lax.fori_loop(0, VARS, send_each(peers[SECOND]), 0)
    pl.semaphore_wait(known.at[1], 4)
    tell(2)
    send(0, peers[THIRD])
    pl.semaphore_wait(known.at[2], 4)
    send(0, peers[14:])
    lax.fori_loop(1, VARS, send_each(peers[10:]), 0)

    index_copy.wait()
    shape = (8, RECORD_LENGTH)
    row = lax.broadcasted_iota(jnp.int32, shape, 0)
    time = lax.broadcasted_iota(jnp.int32, shape, 1)
    windows = []
    for b in range(SEGMENT_NUMBER):
        lag = time - HOP * b
        window = jnp.float32(0.5) - jnp.float32(0.5) * cosine(lag)
        window = jnp.where((lag >= 0) & (lag < BLK), window, jnp.float32(0.0))
        windows.append(window / jnp.sqrt(jnp.float32(3.0 * BLK / 8.0)))

    def fill(g, carry):
        index = jnp.full(shape, idx_ref[8 * g], jnp.int32)
        for i in range(1, 8):
            index = jnp.where(row == i, idx_ref[8 * g + i], index)
        for b in range(SEGMENT_NUMBER):
            phase = index * (time - HOP * b)
            for c in range(2):
                rows = pl.ds(pl.multiple_of(64 * c + 32 * b + 8 * g, 8), 8)
                multipliers[rows, :] = cosine(phase + (BLK // 4) * c) * windows[b]
        return carry

    lax.fori_loop(0, RETAINED_MODES // 8, fill, 0)
    twiddles[...] = multipliers[...].astype(jnp.bfloat16)
    sums[...] = jnp.zeros_like(sums)
    weight_copy.wait()
    root = jnp.sqrt(w_ref[...])
    for c in range(2):
        roots[pl.ds(c, groups * tiles, stride=2), :] = root

    @pl.when(place == 0)
    def _():
        pl.semaphore_wait(here, n_planes)
        for p, z in planes:
            pl.semaphore_signal(everyone, inc=1, device_id={"px": p, "py": z}, device_id_type=MESH)

    def transform(v):
        pltpu.make_async_copy(arrived.at[v, pl.ds(0, n)], arrived.at[v, pl.ds(0, n)], recv_sem.at[v]).wait()
        pltpu.make_async_copy(snap.at[v, :, own], arrived.at[v, me], own_sem.at[v]).wait()
        series = arrived[v].reshape(RECORD_LENGTH, width)
        raw = jnp.dot(twiddles[...], series, preferred_element_type=jnp.float32)
        terms[...] = raw
        for j in range(tiles):
            for b in range(SEGMENT_NUMBER):
                for c in range(2):
                    first = 64 * c + 32 * b
                    part = raw[first : first + RETAINED_MODES, j * LANES : (j + 1) * LANES]
                    turned[pl.ds(8 * b + 2 * j + c, RETAINED_MODES, stride=16), :] = part
        staged[v] = turned[...].astype(jnp.bfloat16).reshape(groups, 4, 8, LANES)
        held[v, me] = staged[v, me]
        total = [sums[i] for i in range(4)]
        for j in range(tiles):
            w = w_ref[pl.ds(me * tiles + j, 1), :]
            cut = slice(j * LANES, (j + 1) * LANES)
            r0, r1, i0, i1 = (terms[32 * i : 32 * i + 32, cut] for i in range(4))
            total[0] += (r0 * r0 + i0 * i0) * w
            total[1] += (r1 * r1 + i1 * i1) * w
            total[2] += (r0 * r1 + i0 * i1) * w
            total[3] += (r0 * i1 - i0 * r1) * w
        for i in range(4):
            sums[i] = total[i]

    def send_back(v):
        for peer in peers:
            pltpu.make_async_remote_copy(
                src_ref=staged.at[v, peer], dst_ref=held.at[v, me], send_sem=send_two.at[v], recv_sem=recv_two.at[v],
                device_id={"ta": peer}, device_id_type=MESH,
            ).start()

    def work(v, carry):
        transform(v)
        send_back(v)
        return carry

    lax.fori_loop(0, VARS - 1, work, 0)
    transform(VARS - 1)

    line = lax.broadcasted_iota(jnp.int32, (8, LANES), 0)
    shape = (RETAINED_MODES, LANES)
    diagonal = lax.broadcasted_iota(jnp.int32, shape, 0) == lax.broadcasted_iota(jnp.int32, shape, 1)
    both = jnp.zeros((8, LANES), jnp.float32)
    for i in range(4):
        column = jnp.sum(sums[i], axis=1, keepdims=True)
        lanes = jnp.sum(jnp.where(diagonal, column, jnp.float32(0.0)), axis=0, keepdims=True)
        both = jnp.where(line == i, lanes, both)
    gram_mine[...] = both

    @pl.when(place != 0)
    def _():
        pl.semaphore_wait(everyone, 1)

    gram_seen[place] = both
    for p, z in planes:
        pltpu.make_async_remote_copy(
            src_ref=gram_mine, dst_ref=gram_seen.at[place], send_sem=gram_send, recv_sem=gram_recv,
            device_id={"px": p, "py": z}, device_id_type=MESH,
        ).start()
    send_back(VARS - 1)

    def scale(v, carry):
        pltpu.make_async_copy(held.at[v, pl.ds(0, n)], held.at[v, pl.ds(0, n)], recv_two.at[v]).wait()
        for k in range(groups):
            by = roots[8 * k : 8 * k + 8, :]
            for i in range(4):
                spectra[i, v, k] = held[v, k, i].astype(jnp.float32) * by
        return carry

    lax.fori_loop(0, 2, scale, 0)
    pltpu.make_async_copy(gram_seen.at[pl.ds(0, n_planes)], gram_seen.at[pl.ds(0, n_planes)], gram_recv).wait()
    whole = jnp.sum(gram_seen[...], axis=0)
    gram_sum[...] = whole
    gram_out[me] = whole
    for peer in peers:
        pltpu.make_async_remote_copy(
            src_ref=gram_sum, dst_ref=gram_out.at[me], send_sem=last_send, recv_sem=last_recv,
            device_id={"ta": peer}, device_id_type=MESH,
        ).start()
    lax.fori_loop(2, VARS, scale, 0)
    pltpu.make_async_copy(gram_out.at[pl.ds(0, n)], gram_out.at[pl.ds(0, n)], last_recv).wait()
    for v in range(VARS):
        pltpu.make_async_copy(arrived.at[v, pl.ds(0, n)], arrived.at[v, pl.ds(0, n)], send_sem.at[v]).wait()
        pltpu.make_async_copy(held.at[v, pl.ds(0, n)], held.at[v, pl.ds(0, n)], send_two.at[v]).wait()
    pltpu.make_async_copy(gram_seen.at[pl.ds(0, n_planes)], gram_seen.at[pl.ds(0, n_planes)], gram_send).wait()
    pltpu.make_async_copy(gram_out.at[pl.ds(0, n)], gram_out.at[pl.ds(0, n)], last_send).wait()


def finish_kernel(total, spectra, gram_in, out, gram, sem):
    copies = [pltpu.make_async_copy(spectra.at[i], out.at[i], sem.at[i]) for i in range(4)]
    for copy in copies:
        copy.start()
    me = lax.axis_index("ta")
    sums = jnp.sum(gram_in[...], axis=0) / jnp.float32(total)
    sums = pltpu.roll(sums, lax.rem(LANES - 2 * me, LANES), 1)
    r = lax.broadcasted_iota(jnp.int32, (2, 2), 0)
    c = lax.broadcasted_iota(jnp.int32, (2, 2), 1)
    zero = jnp.zeros((2, 2), jnp.float32)
    for f in range(2):
        first, second, real, imag = (jnp.broadcast_to(sums[i : i + 1, f : f + 1], (2, 2)) for i in range(4))
        for b in range(2):
            power = jnp.where(c == 0, second if b else first, zero)
            gram[f, b] = jnp.where(r == b, power, jnp.where(c == 0, real, -imag if b else imag))
    for copy in copies:
        copy.wait()


def solution(mesh):
    groups, cores, depth = mesh.shape["ta"], mesh.shape["px"], mesh.shape["py"]

    def on_device(snapshots, quad_weights, spectral_indices):
        steps, _, points = snapshots.shape
        width = points // groups
        series = jnp.transpose(snapshots, (1, 0, 2))
        weights = quad_weights.reshape(points // LANES, LANES)
        hbm = pl.BlockSpec(memory_space=pltpu.HBM)
        vmem = pl.BlockSpec(memory_space=pltpu.VMEM)
        spectra, gram_parts = pl.pallas_call(
            functools.partial(exchange_kernel, groups, width, cores, depth),
            name="exchange",
            out_shape=(
                jax.ShapeDtypeStruct((4, VARS, groups, 8, LANES), jnp.float32),
                jax.ShapeDtypeStruct((groups, 8, LANES), jnp.float32),
            ),
            in_specs=[hbm, hbm, hbm],
            out_specs=(vmem, vmem),
            scratch_shapes=[
                pltpu.VMEM((VARS, steps, points), jnp.bfloat16),
                pltpu.VMEM((VARS, groups, steps, width), jnp.bfloat16),
                pltpu.VMEM((ROWS, RECORD_LENGTH), jnp.float32),
                pltpu.VMEM((ROWS, RECORD_LENGTH), jnp.bfloat16),
                pltpu.VMEM((ROWS, width), jnp.float32),
                pltpu.VMEM((ROWS * width // LANES, LANES), jnp.float32),
                pltpu.VMEM((VARS, groups, 4, 8, LANES), jnp.bfloat16),
                pltpu.VMEM((VARS, groups, 4, 8, LANES), jnp.bfloat16),
                pltpu.VMEM((points // LANES, LANES), jnp.float32),
                pltpu.VMEM((2 * points // LANES, LANES), jnp.float32),
                pltpu.SMEM((RETAINED_MODES,), jnp.int32),
                pltpu.VMEM((4, RETAINED_MODES, LANES), jnp.float32),
                pltpu.VMEM((8, LANES), jnp.float32),
                pltpu.VMEM((cores * depth, 8, LANES), jnp.float32),
                pltpu.VMEM((8, LANES), jnp.float32),
                pltpu.SemaphoreType.DMA((VARS,)),
                pltpu.SemaphoreType.DMA((VARS,)),
                pltpu.SemaphoreType.DMA((2,)),
                pltpu.SemaphoreType.DMA((VARS,)),
                pltpu.SemaphoreType.DMA((VARS,)),
                pltpu.SemaphoreType.DMA((VARS,)),
                pltpu.SemaphoreType.DMA((VARS,)),
                pltpu.SemaphoreType.DMA,
                pltpu.SemaphoreType.DMA,
                pltpu.SemaphoreType.DMA,
                pltpu.SemaphoreType.DMA,
                pltpu.SemaphoreType.REGULAR((3,)),
                pltpu.SemaphoreType.REGULAR,
                pltpu.SemaphoreType.REGULAR,
            ],
            compiler_params=pltpu.CompilerParams(collective_id=0, has_side_effects=True, vmem_limit_bytes=32 * 2**20),
        )(*(pltpu.with_memory_space_constraint(a, pltpu.HBM) for a in (series, weights, spectral_indices)))
        total = points * cores * depth * VARS
        spectra, gram = pl.pallas_call(
            functools.partial(finish_kernel, total),
            name="finish",
            out_shape=(
                jax.ShapeDtypeStruct((4, VARS, groups, 8, LANES), jnp.float32),
                jax.ShapeDtypeStruct((2, 2, 2, 2), jnp.float32),
            ),
            in_specs=[vmem, vmem],
            out_specs=(hbm, vmem),
            scratch_shapes=[pltpu.SemaphoreType.DMA((4,))],
            compiler_params=pltpu.CompilerParams(vmem_limit_bytes=8 * 2**20),
        )(spectra, gram_parts)
        spectra = spectra.reshape(2, SEGMENT_NUMBER, VARS, groups, width // LANES, 2, LANES)
        spectra = spectra.transpose(0, 1, 5, 2, 3, 4, 6).reshape(2, SEGMENT_NUMBER, 2, VARS, points)
        return (spectra, gram)

    return jax.shard_map(
        on_device,
        mesh=mesh,
        in_specs=(P("ta", None, ("px", "py")), P(("px", "py")), P()),
        out_specs=(P("ta", None, None, None, ("px", "py")), P("ta", None, None, None)),
        check_vma=False,
    )
```

```python
import functools
import math

import jax
import jax.numpy as jnp
from jax import lax
from jax.experimental import pallas as pl
from jax.experimental.pallas import tpu as pltpu
from jax.sharding import PartitionSpec as P

VARS = 5
BLK = 256
HOP = 128
SEGMENT_NUMBER = 2
RECORD_LENGTH = 384
RETAINED_MODES = 32
ROWS = RETAINED_MODES * SEGMENT_NUMBER * 2
MESH = pl.DeviceIdType.MESH
LANES = 128
STEPS = (
    (0, 1), (0, 3), (1, 0), (3, 0), (0, 2), (2, 0), (1, 1), (3, 3),
    (1, 3), (3, 1), (2, 1), (2, 3), (1, 2), (3, 2), (2, 2),
)
NEAR, SECOND, THIRD = slice(0, 4), slice(4, 10), slice(10, 14)


def cosine(phase):
    k = jnp.bitwise_and(phase, BLK - 1)
    k = jnp.where(k > BLK // 2, BLK - k, k)
    far = k > BLK // 4
    k = jnp.where(far, BLK // 2 - k, k)
    a = k.astype(jnp.float32) * jnp.float32(2.0 * math.pi / BLK)
    s = a * a
    total = jnp.float32(1.0 / math.factorial(12))
    for n in (10, 8, 6, 4, 2, 0):
        total = total * s * -1.0 if n == 10 else total * s
        total = total + jnp.float32((-1.0) ** (n // 2) / math.factorial(n))
    return jnp.where(far, -total, total)


def exchange_kernel(
    groups, width, cores, depth,
    snap, weights, indices, spectra, gram_out,
    mine, arrived, multipliers, twiddles, terms, turned, staged, held, w_ref, roots, idx_ref, sums, gram_mine, gram_seen, gram_sum,
    load_sem, own_sem, small_sem, send_sem, recv_sem, send_two, recv_two, gram_send, gram_recv, last_send, last_recv, known, here, everyone,
):
    me = lax.axis_index("ta")
    px, py = lax.axis_index("px"), lax.axis_index("py")
    side = math.isqrt(groups)
    y, x = me // side, me % side
    peers = [lax.rem(y + dy, side) * side + lax.rem(x + dx, side) for dy, dx in STEPS]
    place = px * depth + py
    others = [(dp, dz) for dz in range(depth) for dp in range(cores) if (dp, dz) != (0, 0)]
    planes = [(lax.rem(px + dp, cores), lax.rem(py + dz, depth)) for dp, dz in others]
    far_planes = [planes[i] for i in sorted(range(len(others)), key=lambda i: -min(others[i][1], depth - others[i][1]))]
    n, n_planes, tiles = len(peers), len(planes), width // LANES

    barrier = pltpu.get_barrier_semaphore()
    for peer in peers[NEAR]:
        pl.semaphore_signal(barrier, inc=1, device_id={"ta": peer}, device_id_type=MESH)

    @pl.when(place == 0)
    def _():
        for p, z in planes:
            pl.semaphore_signal(barrier, inc=1, device_id={"px": p, "py": z}, device_id_type=MESH)

    loads = [pltpu.make_async_copy(snap.at[v], mine.at[v], load_sem.at[v]) for v in range(VARS)]
    for load in loads:
        load.start()
    index_copy = pltpu.make_async_copy(indices, idx_ref, small_sem.at[0])
    index_copy.start()
    weight_copy = pltpu.make_async_copy(weights, w_ref, small_sem.at[1])
    weight_copy.start()
    own = pl.ds(pl.multiple_of(me * width, LANES), width)
    for v in range(VARS):
        pltpu.make_async_copy(snap.at[v, :, own], arrived.at[v, me], own_sem.at[v]).start()

    pl.semaphore_wait(barrier, jnp.where(place == 0, 4, 5))

    def tell(i):
        for peer in peers[NEAR]:
            pl.semaphore_signal(known.at[i], inc=1, device_id={"ta": peer}, device_id_type=MESH)

    def send(v, to):
        for peer in to:
            cut = pl.ds(pl.multiple_of(peer * width, LANES), width)
            pltpu.make_async_remote_copy(
                src_ref=mine.at[v, :, cut], dst_ref=arrived.at[v, me], send_sem=send_sem.at[v], recv_sem=recv_sem.at[v],
                device_id={"ta": peer}, device_id_type=MESH,
            ).start()

    def send_each(to):
        def step(v, carry):
            send(v, to)
            return carry

        return step

    tell(0)

    @pl.when(place != 0)
    def _():
        pl.semaphore_signal(here, inc=1, device_id={"px": 0, "py": 0}, device_id_type=MESH)

    for v in range(VARS - 1):
        loads[v].wait()
        send(v, peers[NEAR])
    loads[VARS - 1].wait()
    pl.semaphore_wait(known.at[0], 4)
    tell(1)
    lax.fori_loop(0, VARS - 1, send_each(peers[SECOND]), 0)
    pl.semaphore_wait(known.at[1], 4)
    tell(2)
    send(0, peers[THIRD])
    pl.semaphore_wait(known.at[2], 4)
    send(0, peers[14:])
    lax.fori_loop(1, VARS - 1, send_each(peers[10:]), 0)
    send(VARS - 1, peers[::-1])

    index_copy.wait()
    shape = (8, RECORD_LENGTH)
    row = lax.broadcasted_iota(jnp.int32, shape, 0)
    time = lax.broadcasted_iota(jnp.int32, shape, 1)
    windows = []
    for b in range(SEGMENT_NUMBER):
        lag = time - HOP * b
        window = jnp.float32(0.5) - jnp.float32(0.5) * cosine(lag)
        window = jnp.where((lag >= 0) & (lag < BLK), window, jnp.float32(0.0))
        windows.append(window / jnp.sqrt(jnp.float32(3.0 * BLK / 8.0)))

    def fill(g, carry):
        index = jnp.full(shape, idx_ref[8 * g], jnp.int32)
        for i in range(1, 8):
            index = jnp.where(row == i, idx_ref[8 * g + i], index)
        for b in range(SEGMENT_NUMBER):
            phase = index * (time - HOP * b)
            for c in range(2):
                rows = pl.ds(pl.multiple_of(64 * c + 32 * b + 8 * g, 8), 8)
                multipliers[rows, :] = cosine(phase + (BLK // 4) * c) * windows[b]
        return carry

    lax.fori_loop(0, RETAINED_MODES // 8, fill, 0)
    twiddles[...] = multipliers[...].astype(jnp.bfloat16)
    sums[...] = jnp.zeros_like(sums)
    weight_copy.wait()
    root = jnp.sqrt(w_ref[...])
    for c in range(2):
        roots[pl.ds(c, groups * tiles, stride=2), :] = root

    @pl.when(place == 0)
    def _():
        pl.semaphore_wait(here, n_planes)
        for p, z in planes:
            pl.semaphore_signal(everyone, inc=1, device_id={"px": p, "py": z}, device_id_type=MESH)

    def transform(v):
        pltpu.make_async_copy(arrived.at[v, pl.ds(0, n)], arrived.at[v, pl.ds(0, n)], recv_sem.at[v]).wait()
        pltpu.make_async_copy(snap.at[v, :, own], arrived.at[v, me], own_sem.at[v]).wait()
        series = arrived[v].reshape(RECORD_LENGTH, width)
        raw = jnp.dot(twiddles[...], series, preferred_element_type=jnp.float32)
        terms[...] = raw
        total = [sums[i] for i in range(4)]
        for j in range(tiles):
            w = w_ref[pl.ds(me * tiles + j, 1), :]
            cut = slice(j * LANES, (j + 1) * LANES)
            r0, r1, i0, i1 = (terms[32 * i : 32 * i + 32, cut] for i in range(4))
            total[0] += (r0 * r0 + i0 * i0) * w
            total[1] += (r1 * r1 + i1 * i1) * w
            total[2] += (r0 * r1 + i0 * i1) * w
            total[3] += (r0 * i1 - i0 * r1) * w
        for i in range(4):
            sums[i] = total[i]

    def lay_out(v):
        for j in range(tiles):
            for b in range(SEGMENT_NUMBER):
                for c in range(2):
                    first = 64 * c + 32 * b
                    part = terms[first : first + RETAINED_MODES, j * LANES : (j + 1) * LANES]
                    turned[pl.ds(8 * b + 2 * j + c, RETAINED_MODES, stride=16), :] = part
        staged[v] = turned[...].astype(jnp.bfloat16).reshape(groups, 4, 8, LANES)
        held[v, me] = staged[v, me]

    def send_back(v):
        for peer in peers[::-1]:
            pltpu.make_async_remote_copy(
                src_ref=staged.at[v, peer], dst_ref=held.at[v, me], send_sem=send_two.at[v], recv_sem=recv_two.at[v],
                device_id={"ta": peer}, device_id_type=MESH,
            ).start()

    def work(v, carry):
        transform(v)
        lay_out(v)
        return carry

    lax.fori_loop(0, VARS - 1, work, 0)
    transform(VARS - 1)

    shape = (RETAINED_MODES, LANES)
    ahead = lax.broadcasted_iota(jnp.int32, shape, 1) - lax.broadcasted_iota(jnp.int32, shape, 0)
    lanes = jnp.zeros(shape, jnp.float32)
    for i in range(4):
        lanes = jnp.where(ahead == RETAINED_MODES * i, jnp.sum(sums[i], axis=1, keepdims=True), lanes)
    lanes = jnp.sum(lanes, axis=0, keepdims=True)
    gram_mine[...] = lanes
    gram_seen[place] = lanes

    @pl.when(place != 0)
    def _():
        pl.semaphore_wait(everyone, 1)

    for p, z in far_planes:
        pltpu.make_async_remote_copy(
            src_ref=gram_mine, dst_ref=gram_seen.at[place], send_sem=gram_send, recv_sem=gram_recv,
            device_id={"px": p, "py": z}, device_id_type=MESH,
        ).start()
    def send_early(v, carry):
        send_back(v)
        return carry

    lax.fori_loop(0, VARS - 1, send_early, 0)
    lay_out(VARS - 1)
    send_back(VARS - 1)

    def scale(v, carry):
        pltpu.make_async_copy(held.at[v, pl.ds(0, n)], held.at[v, pl.ds(0, n)], recv_two.at[v]).wait()
        for k in range(groups):
            by = roots[8 * k : 8 * k + 8, :]
            for i in range(4):
                spectra[i, v, k] = held[v, k, i].astype(jnp.float32) * by
        return carry

    lax.fori_loop(0, 2, scale, 0)
    pltpu.make_async_copy(gram_seen.at[pl.ds(0, n_planes)], gram_seen.at[pl.ds(0, n_planes)], gram_recv).wait()
    whole = jnp.sum(gram_seen[...], axis=0)
    gram_sum[...] = whole
    gram_out[me] = whole
    for peer in peers[::-1]:
        pltpu.make_async_remote_copy(
            src_ref=gram_sum, dst_ref=gram_out.at[me], send_sem=last_send, recv_sem=last_recv,
            device_id={"ta": peer}, device_id_type=MESH,
        ).start()
    lax.fori_loop(2, VARS, scale, 0)
    pltpu.make_async_copy(gram_out.at[pl.ds(0, n)], gram_out.at[pl.ds(0, n)], last_recv).wait()
    for v in range(VARS):
        pltpu.make_async_copy(arrived.at[v, pl.ds(0, n)], arrived.at[v, pl.ds(0, n)], send_sem.at[v]).wait()
        pltpu.make_async_copy(held.at[v, pl.ds(0, n)], held.at[v, pl.ds(0, n)], send_two.at[v]).wait()
    pltpu.make_async_copy(gram_seen.at[pl.ds(0, n_planes)], gram_seen.at[pl.ds(0, n_planes)], gram_send).wait()
    pltpu.make_async_copy(gram_out.at[pl.ds(0, n)], gram_out.at[pl.ds(0, n)], last_send).wait()


def finish_kernel(total, spectra, gram_in, out, gram_out, gram, sem):
    copies = [pltpu.make_async_copy(spectra.at[i], out.at[i], sem.at[i]) for i in range(4)]
    for copy in copies:
        copy.start()
    me = lax.axis_index("ta")
    sums = jnp.sum(gram_in[...], axis=0) / jnp.float32(total)
    sums = pltpu.roll(sums, lax.rem(LANES - 2 * me, LANES), 1)
    r = lax.broadcasted_iota(jnp.int32, (2, 2), 0)
    c = lax.broadcasted_iota(jnp.int32, (2, 2), 1)
    zero = jnp.zeros((2, 2), jnp.float32)
    for f in range(2):
        first, second, real, imag = (jnp.broadcast_to(sums[:, RETAINED_MODES * i + f : RETAINED_MODES * i + f + 1], (2, 2)) for i in range(4))
        for b in range(2):
            power = jnp.where(c == 0, second if b else first, zero)
            gram[f, b] = jnp.where(r == b, power, jnp.where(c == 0, real, -imag if b else imag))
    copies.append(pltpu.make_async_copy(gram, gram_out, sem.at[4]))
    copies[-1].start()
    for copy in copies:
        copy.wait()


def solution(mesh):
    groups, cores, depth = mesh.shape["ta"], mesh.shape["px"], mesh.shape["py"]

    def on_device(snapshots, quad_weights, spectral_indices):
        steps, _, points = snapshots.shape
        width = points // groups
        series = jnp.transpose(snapshots, (1, 0, 2))
        weights = quad_weights.reshape(points // LANES, LANES)
        hbm = pl.BlockSpec(memory_space=pltpu.HBM)
        vmem = pl.BlockSpec(memory_space=pltpu.VMEM)
        spectra, gram_parts = pl.pallas_call(
            functools.partial(exchange_kernel, groups, width, cores, depth),
            name="exchange",
            out_shape=(
                jax.ShapeDtypeStruct((4, VARS, groups, 8, LANES), jnp.float32),
                jax.ShapeDtypeStruct((groups, 1, LANES), jnp.float32),
            ),
            in_specs=[hbm, hbm, hbm],
            out_specs=(vmem, vmem),
            scratch_shapes=[
                pltpu.VMEM((VARS, steps, points), jnp.bfloat16),
                pltpu.VMEM((VARS, groups, steps, width), jnp.bfloat16),
                pltpu.VMEM((ROWS, RECORD_LENGTH), jnp.float32),
                pltpu.VMEM((ROWS, RECORD_LENGTH), jnp.bfloat16),
                pltpu.VMEM((ROWS, width), jnp.float32),
                pltpu.VMEM((ROWS * width // LANES, LANES), jnp.float32),
                pltpu.VMEM((VARS, groups, 4, 8, LANES), jnp.bfloat16),
                pltpu.VMEM((VARS, groups, 4, 8, LANES), jnp.bfloat16),
                pltpu.VMEM((points // LANES, LANES), jnp.float32),
                pltpu.VMEM((2 * points // LANES, LANES), jnp.float32),
                pltpu.SMEM((RETAINED_MODES,), jnp.int32),
                pltpu.VMEM((4, RETAINED_MODES, LANES), jnp.float32),
                pltpu.VMEM((1, LANES), jnp.float32),
                pltpu.VMEM((cores * depth, 1, LANES), jnp.float32),
                pltpu.VMEM((1, LANES), jnp.float32),
                pltpu.SemaphoreType.DMA((VARS,)),
                pltpu.SemaphoreType.DMA((VARS,)),
                pltpu.SemaphoreType.DMA((2,)),
                pltpu.SemaphoreType.DMA((VARS,)),
                pltpu.SemaphoreType.DMA((VARS,)),
                pltpu.SemaphoreType.DMA((VARS,)),
                pltpu.SemaphoreType.DMA((VARS,)),
                pltpu.SemaphoreType.DMA,
                pltpu.SemaphoreType.DMA,
                pltpu.SemaphoreType.DMA,
                pltpu.SemaphoreType.DMA,
                pltpu.SemaphoreType.REGULAR((3,)),
                pltpu.SemaphoreType.REGULAR,
                pltpu.SemaphoreType.REGULAR,
            ],
            compiler_params=pltpu.CompilerParams(collective_id=0, has_side_effects=True, vmem_limit_bytes=32 * 2**20),
        )(*(pltpu.with_memory_space_constraint(a, pltpu.HBM) for a in (series, weights, spectral_indices)))
        total = points * cores * depth * VARS
        spectra, gram = pl.pallas_call(
            functools.partial(finish_kernel, total),
            name="finish",
            out_shape=(
                jax.ShapeDtypeStruct((4, VARS, groups, 8, LANES), jnp.float32),
                jax.ShapeDtypeStruct((2, 2, 2, 2), jnp.float32),
            ),
            in_specs=[vmem, vmem],
            out_specs=(hbm, hbm),
            scratch_shapes=[pltpu.VMEM((2, 2, 2, 2), jnp.float32), pltpu.SemaphoreType.DMA((5,))],
            compiler_params=pltpu.CompilerParams(vmem_limit_bytes=8 * 2**20),
        )(spectra, gram_parts)
        spectra = spectra.reshape(2, SEGMENT_NUMBER, VARS, groups, width // LANES, 2, LANES)
        spectra = spectra.transpose(0, 1, 5, 2, 3, 4, 6).reshape(2, SEGMENT_NUMBER, 2, VARS, points)
        return (spectra, gram)

    return jax.shard_map(
        on_device,
        mesh=mesh,
        in_specs=(P("ta", None, ("px", "py")), P(("px", "py")), P()),
        out_specs=(P("ta", None, None, None, ("px", "py")), P("ta", None, None, None)),
        check_vma=False,
    )
```

```python
import functools
import math

import jax
import jax.numpy as jnp
from jax import lax
from jax.experimental import pallas as pl
from jax.experimental.pallas import tpu as pltpu
from jax.sharding import PartitionSpec as P

VARS = 5
BLK = 256
HOP = 128
SEGMENT_NUMBER = 2
RECORD_LENGTH = 384
RETAINED_MODES = 32
ROWS = RETAINED_MODES * SEGMENT_NUMBER * 2
MESH = pl.DeviceIdType.MESH
LANES = 128
BORROWED = 128
STEPS = (
    (0, 1), (0, 3), (1, 0), (3, 0), (0, 2), (2, 0), (1, 1), (3, 3),
    (1, 3), (3, 1), (2, 1), (2, 3), (1, 2), (3, 2), (2, 2),
)
NEAR, SECOND, THIRD = slice(0, 4), slice(4, 10), slice(10, 14)


def cosine(phase):
    k = jnp.bitwise_and(phase, BLK - 1)
    k = jnp.where(k > BLK // 2, BLK - k, k)
    far = k > BLK // 4
    k = jnp.where(far, BLK // 2 - k, k)
    a = k.astype(jnp.float32) * jnp.float32(2.0 * math.pi / BLK)
    s = a * a
    total = jnp.float32(1.0 / math.factorial(12))
    for n in (10, 8, 6, 4, 2, 0):
        total = total * s * -1.0 if n == 10 else total * s
        total = total + jnp.float32((-1.0) ** (n // 2) / math.factorial(n))
    return jnp.where(far, -total, total)


def exchange_kernel(
    groups, width, cores, depth,
    snap, weights, indices, spectra, gram_out,
    mine, arrived, multipliers, twiddles, terms, turned, staged, held, w_ref, roots, idx_ref, sums, gram_mine, gram_seen, gram_sum,
    load_sem, own_sem, small_sem, send_sem, recv_sem, send_two, recv_two, gram_send, gram_recv, last_send, last_recv, known, here, everyone, relay, relay_sem,
):
    me = lax.axis_index("ta")
    side = math.isqrt(groups)
    y, x = me // side, me % side

    def member(step):
        return lax.rem(y + step[0], side) * side + lax.rem(x + step[1], side)

    barrier = pltpu.get_barrier_semaphore()
    peers = [member(step) for step in STEPS[NEAR]]
    for peer in peers:
        pl.semaphore_signal(barrier, inc=1, device_id={"ta": peer}, device_id_type=MESH)
    loads = [pltpu.make_async_copy(snap.at[v], mine.at[v], load_sem.at[v]) for v in range(VARS)]
    for load in loads:
        load.start()
    px, py = lax.axis_index("px"), lax.axis_index("py")
    late, partner = py >= depth // 2, depth - 1 - py
    last = VARS - 1
    place = px * depth + py
    others = [(dp, dz) for dz in range(depth) for dp in range(cores) if (dp, dz) != (0, 0)]

    @pl.when(place == 0)
    def _():
        for p, z in others:
            pl.semaphore_signal(barrier, inc=1, device_id={"px": p, "py": z}, device_id_type=MESH)

    @pl.when(jnp.logical_not(late))
    def _():
        pl.semaphore_signal(barrier, inc=1, device_id={"py": partner}, device_id_type=MESH)

    peers += [member(step) for step in STEPS[NEAR.stop :]]
    planes = [(lax.rem(px + dp, cores), lax.rem(py + dz, depth)) for dp, dz in others]
    far_planes = [planes[i] for i in sorted(range(len(others)), key=lambda i: -min(others[i][1], depth - others[i][1]))]
    n, n_planes, tiles = len(peers), len(planes), width // LANES
    index_copy = pltpu.make_async_copy(indices, idx_ref, small_sem.at[0])
    index_copy.start()
    weight_copy = pltpu.make_async_copy(weights, w_ref, small_sem.at[1])
    weight_copy.start()
    own = pl.ds(pl.multiple_of(me * width, LANES), width)
    kept = pl.ds(BORROWED, width - BORROWED)
    for v in range(last):
        pltpu.make_async_copy(snap.at[v, :, own], arrived.at[v, me], own_sem.at[v]).start()

    def own_last():
        cut = pl.ds(pl.multiple_of(me * width + BORROWED, LANES), width - BORROWED)
        return pltpu.make_async_copy(snap.at[last, :, cut], arrived.at[last, me, :, kept], own_sem.at[last])

    def own_whole(v):
        return pltpu.make_async_copy(snap.at[v, :, own], arrived.at[v, me], own_sem.at[v])

    @pl.when(late)
    def _():
        own_last().start()

    @pl.when(jnp.logical_not(late))
    def _():
        own_whole(last).start()

    pl.semaphore_wait(barrier, jnp.where(place == 0, 4, jnp.where(late, 6, 5)))

    def tell(i):
        for peer in peers[NEAR]:
            pl.semaphore_signal(known.at[i], inc=1, device_id={"ta": peer}, device_id_type=MESH)

    def send(v, to):
        for peer in to:
            cut = pl.ds(pl.multiple_of(peer * width, LANES), width)
            pltpu.make_async_remote_copy(
                src_ref=mine.at[v, :, cut], dst_ref=arrived.at[v, me], send_sem=send_sem.at[v], recv_sem=recv_sem.at[v],
                device_id={"ta": peer}, device_id_type=MESH,
            ).start()

    def send_each(to):
        def step(v, carry):
            send(v, to)
            return carry

        return step

    tell(0)

    @pl.when(place != 0)
    def _():
        pl.semaphore_signal(here, inc=1, device_id={"px": 0, "py": 0}, device_id_type=MESH)

    for v in range(VARS - 1):
        loads[v].wait()
        send(v, peers[NEAR])
    loads[VARS - 1].wait()
    pl.semaphore_wait(known.at[0], 4)
    tell(1)
    lax.fori_loop(0, VARS - 1, send_each(peers[SECOND]), 0)
    pl.semaphore_wait(known.at[1], 4)
    tell(2)
    send(0, peers[THIRD])
    pl.semaphore_wait(known.at[2], 4)
    tell(3)
    send(0, peers[14:])
    pl.semaphore_wait(known.at[3], 4)

    @pl.when(late)
    def _():
        for peer in [*peers[::-1], me]:
            cut = pl.ds(pl.multiple_of(peer * width, LANES), BORROWED)
            pltpu.make_async_remote_copy(
                src_ref=mine.at[last, :, cut], dst_ref=relay.at[me], send_sem=relay_sem.at[0], recv_sem=relay_sem.at[1],
                device_id={"ta": peer, "py": partner}, device_id_type=MESH,
            ).start()

    lax.fori_loop(1, VARS - 1, send_each(peers[10:]), 0)

    @pl.when(late)
    def _():
        for peer in peers[::-1]:
            cut = pl.ds(pl.multiple_of(peer * width + BORROWED, LANES), width - BORROWED)
            pltpu.make_async_remote_copy(
                src_ref=mine.at[last, :, cut], dst_ref=arrived.at[last, me, :, kept],
                send_sem=send_sem.at[last], recv_sem=recv_sem.at[last],
                device_id={"ta": peer}, device_id_type=MESH,
            ).start()

    @pl.when(jnp.logical_not(late))
    def _():
        send(last, peers[::-1])

    index_copy.wait()
    shape = (8, RECORD_LENGTH)
    row = lax.broadcasted_iota(jnp.int32, shape, 0)
    time = lax.broadcasted_iota(jnp.int32, shape, 1)
    windows = []
    for b in range(SEGMENT_NUMBER):
        lag = time - HOP * b
        window = jnp.float32(0.5) - jnp.float32(0.5) * cosine(lag)
        window = jnp.where((lag >= 0) & (lag < BLK), window, jnp.float32(0.0))
        windows.append(window / jnp.sqrt(jnp.float32(3.0 * BLK / 8.0)))

    def fill(g, carry):
        index = jnp.full(shape, idx_ref[8 * g], jnp.int32)
        for i in range(1, 8):
            index = jnp.where(row == i, idx_ref[8 * g + i], index)
        for b in range(SEGMENT_NUMBER):
            phase = index * (time - HOP * b)
            for c in range(2):
                rows = pl.ds(pl.multiple_of(64 * c + 32 * b + 8 * g, 8), 8)
                multipliers[rows, :] = cosine(phase + (BLK // 4) * c) * windows[b]
        return carry

    lax.fori_loop(0, RETAINED_MODES // 8, fill, 0)
    twiddles[...] = multipliers[...].astype(jnp.bfloat16)
    sums[...] = jnp.zeros_like(sums)
    weight_copy.wait()
    root = jnp.sqrt(w_ref[...])
    for c in range(2):
        roots[pl.ds(c, groups * tiles, stride=2), :] = root

    @pl.when(place == 0)
    def _():
        pl.semaphore_wait(here, n_planes)
        for p, z in others:
            pl.semaphore_signal(everyone, inc=1, device_id={"px": p, "py": z}, device_id_type=MESH)

    def arrive(v):
        pltpu.make_async_copy(arrived.at[v, pl.ds(0, n)], arrived.at[v, pl.ds(0, n)], recv_sem.at[v]).wait()
        own_whole(v).wait()

    def parts_of_last():
        return arrived.at[last, pl.ds(0, n), :, kept]

    def transform(v):
        series = arrived[v].reshape(RECORD_LENGTH, width)
        raw = jnp.dot(twiddles[...], series, preferred_element_type=jnp.float32)
        terms[...] = raw
        total = [sums[i] for i in range(4)]
        for j in range(tiles):
            w = w_ref[pl.ds(me * tiles + j, 1), :]
            cut = slice(j * LANES, (j + 1) * LANES)
            r0, r1, i0, i1 = (terms[32 * i : 32 * i + 32, cut] for i in range(4))
            total[0] += (r0 * r0 + i0 * i0) * w
            total[1] += (r1 * r1 + i1 * i1) * w
            total[2] += (r0 * r1 + i0 * i1) * w
            total[3] += (r0 * i1 - i0 * r1) * w
        for i in range(4):
            sums[i] = total[i]

    def lay_out(v):
        for j in range(tiles):
            for b in range(SEGMENT_NUMBER):
                for c in range(2):
                    first = 64 * c + 32 * b
                    part = terms[first : first + RETAINED_MODES, j * LANES : (j + 1) * LANES]
                    turned[pl.ds(8 * b + 2 * j + c, RETAINED_MODES, stride=16), :] = part
        staged[v] = turned[...].astype(jnp.bfloat16).reshape(groups, 4, 8, LANES)
        held[v, me] = staged[v, me]

    def send_back(v):
        for peer in peers[::-1]:
            pltpu.make_async_remote_copy(
                src_ref=staged.at[v, peer], dst_ref=held.at[v, me], send_sem=send_two.at[v], recv_sem=recv_two.at[v],
                device_id={"ta": peer}, device_id_type=MESH,
            ).start()

    def work(v, carry):
        arrive(v)
        transform(v)
        lay_out(v)
        return carry

    @pl.when(jnp.logical_not(late))
    def _():
        pltpu.make_async_copy(relay, relay, relay_sem.at[1]).wait()
        pltpu.make_async_remote_copy(
            src_ref=relay, dst_ref=arrived.at[last, :, :, pl.ds(0, BORROWED)],
            send_sem=relay_sem.at[2], recv_sem=relay_sem.at[3],
            device_id={"py": partner}, device_id_type=MESH,
        ).start()

    lax.fori_loop(0, VARS - 1, work, 0)

    @pl.when(late)
    def _():
        own_last().wait()
        pltpu.make_async_copy(parts_of_last(), parts_of_last(), recv_sem.at[last]).wait()
        pltpu.make_async_copy(relay, relay, relay_sem.at[3]).wait()

    @pl.when(jnp.logical_not(late))
    def _():
        arrive(last)

    transform(last)

    shape = (RETAINED_MODES, LANES)
    ahead = lax.broadcasted_iota(jnp.int32, shape, 1) - lax.broadcasted_iota(jnp.int32, shape, 0)
    lanes = jnp.zeros(shape, jnp.float32)
    for i in range(4):
        lanes = jnp.where(ahead == RETAINED_MODES * i, jnp.sum(sums[i], axis=1, keepdims=True), lanes)
    lanes = jnp.sum(lanes, axis=0, keepdims=True)
    gram_mine[...] = lanes
    gram_seen[place] = lanes

    @pl.when(place != 0)
    def _():
        pl.semaphore_wait(everyone, 1)

    for p, z in far_planes:
        pltpu.make_async_remote_copy(
            src_ref=gram_mine, dst_ref=gram_seen.at[place], send_sem=gram_send, recv_sem=gram_recv,
            device_id={"px": p, "py": z}, device_id_type=MESH,
        ).start()
    def send_early(v, carry):
        send_back(v)
        return carry

    lax.fori_loop(0, VARS - 1, send_early, 0)
    lay_out(VARS - 1)
    send_back(VARS - 1)

    def scale(v, carry):
        pltpu.make_async_copy(held.at[v, pl.ds(0, n)], held.at[v, pl.ds(0, n)], recv_two.at[v]).wait()
        for k in range(groups):
            by = roots[8 * k : 8 * k + 8, :]
            for i in range(4):
                spectra[i, v, k] = held[v, k, i].astype(jnp.float32) * by
        return carry

    lax.fori_loop(0, 2, scale, 0)
    pltpu.make_async_copy(gram_seen.at[pl.ds(0, n_planes)], gram_seen.at[pl.ds(0, n_planes)], gram_recv).wait()
    whole = jnp.sum(gram_seen[...], axis=0)
    gram_sum[...] = whole
    gram_out[me] = whole
    for peer in peers[::-1]:
        pltpu.make_async_remote_copy(
            src_ref=gram_sum, dst_ref=gram_out.at[me], send_sem=last_send, recv_sem=last_recv,
            device_id={"ta": peer}, device_id_type=MESH,
        ).start()
    lax.fori_loop(2, VARS, scale, 0)
    pltpu.make_async_copy(gram_out.at[pl.ds(0, n)], gram_out.at[pl.ds(0, n)], last_recv).wait()
    for v in range(last):
        pltpu.make_async_copy(arrived.at[v, pl.ds(0, n)], arrived.at[v, pl.ds(0, n)], send_sem.at[v]).wait()

    @pl.when(late)
    def _():
        pltpu.make_async_copy(parts_of_last(), parts_of_last(), send_sem.at[last]).wait()
        pltpu.make_async_copy(relay, relay, relay_sem.at[0]).wait()

    @pl.when(jnp.logical_not(late))
    def _():
        pltpu.make_async_copy(arrived.at[last, pl.ds(0, n)], arrived.at[last, pl.ds(0, n)], send_sem.at[last]).wait()
        pltpu.make_async_copy(relay, relay, relay_sem.at[2]).wait()

    for v in range(VARS):
        pltpu.make_async_copy(held.at[v, pl.ds(0, n)], held.at[v, pl.ds(0, n)], send_two.at[v]).wait()
    pltpu.make_async_copy(gram_seen.at[pl.ds(0, n_planes)], gram_seen.at[pl.ds(0, n_planes)], gram_send).wait()
    pltpu.make_async_copy(gram_out.at[pl.ds(0, n)], gram_out.at[pl.ds(0, n)], last_send).wait()


def finish_kernel(total, spectra, gram_in, out, gram_out, gram, sem):
    copies = [pltpu.make_async_copy(spectra.at[i], out.at[i], sem.at[i]) for i in range(4)]
    for copy in copies:
        copy.start()
    me = lax.axis_index("ta")
    sums = jnp.sum(gram_in[...], axis=0) / jnp.float32(total)
    sums = pltpu.roll(sums, lax.rem(LANES - 2 * me, LANES), 1)
    r = lax.broadcasted_iota(jnp.int32, (2, 2), 0)
    c = lax.broadcasted_iota(jnp.int32, (2, 2), 1)
    zero = jnp.zeros((2, 2), jnp.float32)
    for f in range(2):
        first, second, real, imag = (jnp.broadcast_to(sums[:, RETAINED_MODES * i + f : RETAINED_MODES * i + f + 1], (2, 2)) for i in range(4))
        for b in range(2):
            power = jnp.where(c == 0, second if b else first, zero)
            gram[f, b] = jnp.where(r == b, power, jnp.where(c == 0, real, -imag if b else imag))
    copies.append(pltpu.make_async_copy(gram, gram_out, sem.at[4]))
    copies[-1].start()
    for copy in copies:
        copy.wait()


def solution(mesh):
    groups, cores, depth = mesh.shape["ta"], mesh.shape["px"], mesh.shape["py"]

    def on_device(snapshots, quad_weights, spectral_indices):
        steps, _, points = snapshots.shape
        width = points // groups
        series = jnp.transpose(snapshots, (1, 0, 2))
        weights = quad_weights.reshape(points // LANES, LANES)
        hbm = pl.BlockSpec(memory_space=pltpu.HBM)
        vmem = pl.BlockSpec(memory_space=pltpu.VMEM)
        spectra, gram_parts = pl.pallas_call(
            functools.partial(exchange_kernel, groups, width, cores, depth),
            name="exchange",
            out_shape=(
                jax.ShapeDtypeStruct((4, VARS, groups, 8, LANES), jnp.float32),
                jax.ShapeDtypeStruct((groups, 1, LANES), jnp.float32),
            ),
            in_specs=[hbm, hbm, hbm],
            out_specs=(vmem, vmem),
            scratch_shapes=[
                pltpu.VMEM((VARS, steps, points), jnp.bfloat16),
                pltpu.VMEM((VARS, groups, steps, width), jnp.bfloat16),
                pltpu.VMEM((ROWS, RECORD_LENGTH), jnp.float32),
                pltpu.VMEM((ROWS, RECORD_LENGTH), jnp.bfloat16),
                pltpu.VMEM((ROWS, width), jnp.float32),
                pltpu.VMEM((ROWS * width // LANES, LANES), jnp.float32),
                pltpu.VMEM((VARS, groups, 4, 8, LANES), jnp.bfloat16),
                pltpu.VMEM((VARS, groups, 4, 8, LANES), jnp.bfloat16),
                pltpu.VMEM((points // LANES, LANES), jnp.float32),
                pltpu.VMEM((2 * points // LANES, LANES), jnp.float32),
                pltpu.SMEM((RETAINED_MODES,), jnp.int32),
                pltpu.VMEM((4, RETAINED_MODES, LANES), jnp.float32),
                pltpu.VMEM((1, LANES), jnp.float32),
                pltpu.VMEM((cores * depth, 1, LANES), jnp.float32),
                pltpu.VMEM((1, LANES), jnp.float32),
                pltpu.SemaphoreType.DMA((VARS,)),
                pltpu.SemaphoreType.DMA((VARS,)),
                pltpu.SemaphoreType.DMA((2,)),
                pltpu.SemaphoreType.DMA((VARS,)),
                pltpu.SemaphoreType.DMA((VARS,)),
                pltpu.SemaphoreType.DMA((VARS,)),
                pltpu.SemaphoreType.DMA((VARS,)),
                pltpu.SemaphoreType.DMA,
                pltpu.SemaphoreType.DMA,
                pltpu.SemaphoreType.DMA,
                pltpu.SemaphoreType.DMA,
                pltpu.SemaphoreType.REGULAR((4,)),
                pltpu.SemaphoreType.REGULAR,
                pltpu.SemaphoreType.REGULAR,
                pltpu.VMEM((groups, steps, BORROWED), jnp.bfloat16),
                pltpu.SemaphoreType.DMA((4,)),
            ],
            compiler_params=pltpu.CompilerParams(collective_id=0, has_side_effects=True, vmem_limit_bytes=32 * 2**20),
        )(*(pltpu.with_memory_space_constraint(a, pltpu.HBM) for a in (series, weights, spectral_indices)))
        total = points * cores * depth * VARS
        spectra, gram = pl.pallas_call(
            functools.partial(finish_kernel, total),
            name="finish",
            out_shape=(
                jax.ShapeDtypeStruct((4, VARS, groups, 8, LANES), jnp.float32),
                jax.ShapeDtypeStruct((2, 2, 2, 2), jnp.float32),
            ),
            in_specs=[vmem, vmem],
            out_specs=(hbm, hbm),
            scratch_shapes=[pltpu.VMEM((2, 2, 2, 2), jnp.float32), pltpu.SemaphoreType.DMA((5,))],
            compiler_params=pltpu.CompilerParams(vmem_limit_bytes=8 * 2**20),
        )(spectra, gram_parts)
        spectra = spectra.reshape(2, SEGMENT_NUMBER, VARS, groups, width // LANES, 2, LANES)
        spectra = spectra.transpose(0, 1, 5, 2, 3, 4, 6).reshape(2, SEGMENT_NUMBER, 2, VARS, points)
        return (spectra, gram)

    return jax.shard_map(
        on_device,
        mesh=mesh,
        in_specs=(P("ta", None, ("px", "py")), P(("px", "py")), P()),
        out_specs=(P("ta", None, None, None, ("px", "py")), P("ta", None, None, None)),
        check_vma=False,
    )
```

```python
import functools
import math

import jax
import jax.numpy as jnp
from jax import lax
from jax.experimental import pallas as pl
from jax.experimental.pallas import tpu as pltpu
from jax.sharding import PartitionSpec as P

VARS = 5
BLK = 256
HOP = 128
SEGMENT_NUMBER = 2
RECORD_LENGTH = 384
RETAINED_MODES = 32
ROWS = RETAINED_MODES * SEGMENT_NUMBER * 2
MESH = pl.DeviceIdType.MESH
LANES = 128
BORROWED = 128
STEPS = (
    (0, 1), (0, 3), (1, 0), (3, 0), (0, 2), (2, 0), (1, 1), (3, 3),
    (1, 3), (3, 1), (2, 1), (2, 3), (1, 2), (3, 2), (2, 2),
)
NEAR, SECOND, THIRD = slice(0, 4), slice(4, 10), slice(10, 14)


def cosine(phase):
    k = jnp.bitwise_and(phase, BLK - 1)
    k = jnp.where(k > BLK // 2, BLK - k, k)
    far = k > BLK // 4
    k = jnp.where(far, BLK // 2 - k, k)
    a = k.astype(jnp.float32) * jnp.float32(2.0 * math.pi / BLK)
    s = a * a
    total = jnp.float32(1.0 / math.factorial(12))
    for n in (10, 8, 6, 4, 2, 0):
        total = total * s * -1.0 if n == 10 else total * s
        total = total + jnp.float32((-1.0) ** (n // 2) / math.factorial(n))
    return jnp.where(far, -total, total)


def exchange_kernel(
    groups, width, cores, depth,
    snap, weights, indices, spectra, gram_out,
    mine, arrived, multipliers, twiddles, terms, turned, staged, held, w_ref, roots, idx_ref, sums, gram_mine, gram_seen, gram_sum,
    load_sem, own_sem, small_sem, send_sem, recv_sem, send_two, recv_two, gram_send, gram_recv, last_send, last_recv, known, here, everyone, relay, relay_sem,
):
    me = lax.axis_index("ta")
    side = math.isqrt(groups)
    y, x = me // side, me % side

    def member(step):
        return lax.rem(y + step[0], side) * side + lax.rem(x + step[1], side)

    barrier = pltpu.get_barrier_semaphore()
    peers = [member(step) for step in STEPS[NEAR]]
    for peer in peers:
        pl.semaphore_signal(barrier, inc=1, device_id={"ta": peer}, device_id_type=MESH)
    loads = [pltpu.make_async_copy(snap.at[v], mine.at[v], load_sem.at[v]) for v in range(VARS)]
    for load in loads:
        load.start()
    px, py = lax.axis_index("px"), lax.axis_index("py")
    late, partner = py >= depth // 2, depth - 1 - py
    last = VARS - 1
    place = px * depth + py
    others = [(dp, dz) for dz in range(depth) for dp in range(cores) if (dp, dz) != (0, 0)]

    @pl.when(place == 0)
    def _():
        for p, z in others:
            pl.semaphore_signal(barrier, inc=1, device_id={"px": p, "py": z}, device_id_type=MESH)

    @pl.when(jnp.logical_not(late))
    def _():
        pl.semaphore_signal(barrier, inc=1, device_id={"py": partner}, device_id_type=MESH)

    peers += [member(step) for step in STEPS[NEAR.stop :]]
    planes = [(lax.rem(px + dp, cores), lax.rem(py + dz, depth)) for dp, dz in others]
    far_planes = [planes[i] for i in sorted(range(len(others)), key=lambda i: -min(others[i][1], depth - others[i][1]))]
    n, n_planes, tiles = len(peers), len(planes), width // LANES
    index_copy = pltpu.make_async_copy(indices, idx_ref, small_sem.at[0])
    index_copy.start()
    weight_copy = pltpu.make_async_copy(weights, w_ref, small_sem.at[1])
    weight_copy.start()
    own = pl.ds(pl.multiple_of(me * width, LANES), width)
    kept = pl.ds(BORROWED, width - BORROWED)
    for v in range(last):
        pltpu.make_async_copy(snap.at[v, :, own], arrived.at[v, me], own_sem.at[v]).start()

    def own_last():
        cut = pl.ds(pl.multiple_of(me * width + BORROWED, LANES), width - BORROWED)
        return pltpu.make_async_copy(snap.at[last, :, cut], arrived.at[last, me, :, kept], own_sem.at[last])

    def own_whole(v):
        return pltpu.make_async_copy(snap.at[v, :, own], arrived.at[v, me], own_sem.at[v])

    @pl.when(late)
    def _():
        own_last().start()

    @pl.when(jnp.logical_not(late))
    def _():
        own_whole(last).start()

    pl.semaphore_wait(barrier, jnp.where(place == 0, 4, jnp.where(late, 6, 5)))

    def tell(i):
        for peer in peers[NEAR]:
            pl.semaphore_signal(known.at[i], inc=1, device_id={"ta": peer}, device_id_type=MESH)

    def send(v, to):
        for peer in to:
            cut = pl.ds(pl.multiple_of(peer * width, LANES), width)
            pltpu.make_async_remote_copy(
                src_ref=mine.at[v, :, cut], dst_ref=arrived.at[v, me], send_sem=send_sem.at[v], recv_sem=recv_sem.at[v],
                device_id={"ta": peer}, device_id_type=MESH,
            ).start()

    def send_each(to):
        def step(v, carry):
            send(v, to)
            return carry

        return step

    tell(0)

    @pl.when(place != 0)
    def _():
        pl.semaphore_signal(here, inc=1, device_id={"px": 0, "py": 0}, device_id_type=MESH)

    for v in range(VARS - 1):
        loads[v].wait()
        send(v, peers[NEAR])
    loads[VARS - 1].wait()
    pl.semaphore_wait(known.at[0], 4)
    tell(1)
    lax.fori_loop(0, VARS - 1, send_each(peers[SECOND]), 0)
    pl.semaphore_wait(known.at[1], 4)
    tell(2)
    send(0, peers[THIRD])
    pl.semaphore_wait(known.at[2], 4)
    tell(3)
    send(0, peers[14:])
    pl.semaphore_wait(known.at[3], 4)

    @pl.when(late)
    def _():
        for peer in [*peers[::-1], me]:
            cut = pl.ds(pl.multiple_of(peer * width, LANES), BORROWED)
            pltpu.make_async_remote_copy(
                src_ref=mine.at[last, :, cut], dst_ref=relay.at[me], send_sem=relay_sem.at[0], recv_sem=relay_sem.at[1],
                device_id={"ta": peer, "py": partner}, device_id_type=MESH,
            ).start()

    lax.fori_loop(1, VARS - 1, send_each(peers[10:]), 0)

    @pl.when(late)
    def _():
        for peer in peers[::-1]:
            cut = pl.ds(pl.multiple_of(peer * width + BORROWED, LANES), width - BORROWED)
            pltpu.make_async_remote_copy(
                src_ref=mine.at[last, :, cut], dst_ref=arrived.at[last, me, :, kept],
                send_sem=send_sem.at[last], recv_sem=recv_sem.at[last],
                device_id={"ta": peer}, device_id_type=MESH,
            ).start()

    @pl.when(jnp.logical_not(late))
    def _():
        send(last, peers[::-1])

    index_copy.wait()
    shape = (8, RECORD_LENGTH)
    row = lax.broadcasted_iota(jnp.int32, shape, 0)
    time = lax.broadcasted_iota(jnp.int32, shape, 1)
    windows = []
    for b in range(SEGMENT_NUMBER):
        lag = time - HOP * b
        window = jnp.float32(0.5) - jnp.float32(0.5) * cosine(lag)
        window = jnp.where((lag >= 0) & (lag < BLK), window, jnp.float32(0.0))
        windows.append(window / jnp.sqrt(jnp.float32(3.0 * BLK / 8.0)))

    def fill(g, carry):
        index = jnp.full(shape, idx_ref[8 * g], jnp.int32)
        for i in range(1, 8):
            index = jnp.where(row == i, idx_ref[8 * g + i], index)
        for b in range(SEGMENT_NUMBER):
            phase = index * (time - HOP * b)
            for c in range(2):
                rows = pl.ds(pl.multiple_of(64 * c + 32 * b + 8 * g, 8), 8)
                multipliers[rows, :] = cosine(phase + (BLK // 4) * c) * windows[b]
        return carry

    lax.fori_loop(0, RETAINED_MODES // 8, fill, 0)
    twiddles[...] = multipliers[...].astype(jnp.bfloat16)
    sums[...] = jnp.zeros_like(sums)
    weight_copy.wait()
    root = jnp.sqrt(w_ref[...])
    for c in range(2):
        roots[pl.ds(c, groups * tiles, stride=2), :] = root

    @pl.when(place == 0)
    def _():
        pl.semaphore_wait(here, n_planes)
        for p, z in others:
            pl.semaphore_signal(everyone, inc=1, device_id={"px": p, "py": z}, device_id_type=MESH)

    def arrive(v):
        pltpu.make_async_copy(arrived.at[v, pl.ds(0, n)], arrived.at[v, pl.ds(0, n)], recv_sem.at[v]).wait()
        own_whole(v).wait()

    def parts_of_last():
        return arrived.at[last, pl.ds(0, n), :, kept]

    def transform(v):
        series = arrived[v].reshape(RECORD_LENGTH, width)
        raw = jnp.dot(twiddles[...], series, preferred_element_type=jnp.float32)
        terms[...] = raw
        total = [sums[i] for i in range(4)]
        for j in range(tiles):
            w = w_ref[pl.ds(me * tiles + j, 1), :]
            cut = slice(j * LANES, (j + 1) * LANES)
            r0, r1, i0, i1 = (raw[32 * i : 32 * i + 32, cut] for i in range(4))
            total[0] += (r0 * r0 + i0 * i0) * w
            total[1] += (r1 * r1 + i1 * i1) * w
            total[2] += (r0 * r1 + i0 * i1) * w
            total[3] += (r0 * i1 - i0 * r1) * w
        for i in range(4):
            sums[i] = total[i]

    def lay_out(v):
        for j in range(tiles):
            for b in range(SEGMENT_NUMBER):
                for c in range(2):
                    first = 64 * c + 32 * b
                    part = terms[first : first + RETAINED_MODES, j * LANES : (j + 1) * LANES]
                    turned[pl.ds(8 * b + 2 * j + c, RETAINED_MODES, stride=16), :] = part
        staged[v] = turned[...].astype(jnp.bfloat16).reshape(groups, 4, 8, LANES)
        held[v, me] = staged[v, me]

    def send_back(v):
        for peer in peers[::-1]:
            pltpu.make_async_remote_copy(
                src_ref=staged.at[v, peer], dst_ref=held.at[v, me], send_sem=send_two.at[v], recv_sem=recv_two.at[v],
                device_id={"ta": peer}, device_id_type=MESH,
            ).start()

    def work(v, carry):
        arrive(v)
        transform(v)
        lay_out(v)
        return carry

    @pl.when(jnp.logical_not(late))
    def _():
        pltpu.make_async_copy(relay, relay, relay_sem.at[1]).wait()
        pltpu.make_async_remote_copy(
            src_ref=relay, dst_ref=arrived.at[last, :, :, pl.ds(0, BORROWED)],
            send_sem=relay_sem.at[2], recv_sem=relay_sem.at[3],
            device_id={"py": partner}, device_id_type=MESH,
        ).start()

    lax.fori_loop(0, VARS - 1, work, 0)

    @pl.when(late)
    def _():
        own_last().wait()
        pltpu.make_async_copy(parts_of_last(), parts_of_last(), recv_sem.at[last]).wait()
        pltpu.make_async_copy(relay, relay, relay_sem.at[3]).wait()

    @pl.when(jnp.logical_not(late))
    def _():
        arrive(last)

    transform(last)

    shape = (RETAINED_MODES, LANES)
    ahead = lax.broadcasted_iota(jnp.int32, shape, 1) - lax.broadcasted_iota(jnp.int32, shape, 0)
    lanes = jnp.zeros(shape, jnp.float32)
    for i in range(4):
        lanes = jnp.where(ahead == RETAINED_MODES * i, jnp.sum(sums[i], axis=1, keepdims=True), lanes)
    lanes = jnp.sum(lanes, axis=0, keepdims=True)
    gram_mine[...] = lanes
    gram_seen[place] = lanes

    @pl.when(place != 0)
    def _():
        pl.semaphore_wait(everyone, 1)

    for p, z in far_planes:
        pltpu.make_async_remote_copy(
            src_ref=gram_mine, dst_ref=gram_seen.at[place], send_sem=gram_send, recv_sem=gram_recv,
            device_id={"px": p, "py": z}, device_id_type=MESH,
        ).start()
    lay_out(last)

    def send_in_turn(v, carry):
        send_back(v)
        return carry

    lax.fori_loop(0, VARS, send_in_turn, 0)

    def scale(v, carry):
        pltpu.make_async_copy(held.at[v, pl.ds(0, n)], held.at[v, pl.ds(0, n)], recv_two.at[v]).wait()
        for k in range(groups):
            by = roots[8 * k : 8 * k + 8, :]
            for i in range(4):
                spectra[i, v, k] = held[v, k, i].astype(jnp.float32) * by
        return carry

    lax.fori_loop(0, 2, scale, 0)
    pltpu.make_async_copy(gram_seen.at[pl.ds(0, n_planes)], gram_seen.at[pl.ds(0, n_planes)], gram_recv).wait()
    whole = jnp.sum(gram_seen[...], axis=0)
    gram_sum[...] = whole
    gram_out[me] = whole
    for peer in peers[::-1]:
        pltpu.make_async_remote_copy(
            src_ref=gram_sum, dst_ref=gram_out.at[me], send_sem=last_send, recv_sem=last_recv,
            device_id={"ta": peer}, device_id_type=MESH,
        ).start()
    lax.fori_loop(2, VARS, scale, 0)
    pltpu.make_async_copy(gram_out.at[pl.ds(0, n)], gram_out.at[pl.ds(0, n)], last_recv).wait()
    for v in range(last):
        pltpu.make_async_copy(arrived.at[v, pl.ds(0, n)], arrived.at[v, pl.ds(0, n)], send_sem.at[v]).wait()

    @pl.when(late)
    def _():
        pltpu.make_async_copy(parts_of_last(), parts_of_last(), send_sem.at[last]).wait()
        pltpu.make_async_copy(relay, relay, relay_sem.at[0]).wait()

    @pl.when(jnp.logical_not(late))
    def _():
        pltpu.make_async_copy(arrived.at[last, pl.ds(0, n)], arrived.at[last, pl.ds(0, n)], send_sem.at[last]).wait()
        pltpu.make_async_copy(relay, relay, relay_sem.at[2]).wait()

    for v in range(VARS):
        pltpu.make_async_copy(held.at[v, pl.ds(0, n)], held.at[v, pl.ds(0, n)], send_two.at[v]).wait()
    pltpu.make_async_copy(gram_seen.at[pl.ds(0, n_planes)], gram_seen.at[pl.ds(0, n_planes)], gram_send).wait()
    pltpu.make_async_copy(gram_out.at[pl.ds(0, n)], gram_out.at[pl.ds(0, n)], last_send).wait()


def finish_kernel(total, spectra, gram_in, out, gram_out, gram, sem):
    copies = [pltpu.make_async_copy(spectra.at[i], out.at[i], sem.at[i]) for i in range(4)]
    for copy in copies:
        copy.start()
    me = lax.axis_index("ta")
    sums = jnp.sum(gram_in[...], axis=0) / jnp.float32(total)
    sums = pltpu.roll(sums, lax.rem(LANES - 2 * me, LANES), 1)
    r = lax.broadcasted_iota(jnp.int32, (2, 2), 0)
    c = lax.broadcasted_iota(jnp.int32, (2, 2), 1)
    zero = jnp.zeros((2, 2), jnp.float32)
    for f in range(2):
        first, second, real, imag = (jnp.broadcast_to(sums[:, RETAINED_MODES * i + f : RETAINED_MODES * i + f + 1], (2, 2)) for i in range(4))
        for b in range(2):
            power = jnp.where(c == 0, second if b else first, zero)
            gram[f, b] = jnp.where(r == b, power, jnp.where(c == 0, real, -imag if b else imag))
    copies.append(pltpu.make_async_copy(gram, gram_out, sem.at[4]))
    copies[-1].start()
    for copy in copies:
        copy.wait()


def solution(mesh):
    groups, cores, depth = mesh.shape["ta"], mesh.shape["px"], mesh.shape["py"]

    def on_device(snapshots, quad_weights, spectral_indices):
        steps, _, points = snapshots.shape
        width = points // groups
        series = jnp.transpose(snapshots, (1, 0, 2))
        weights = quad_weights.reshape(points // LANES, LANES)
        hbm = pl.BlockSpec(memory_space=pltpu.HBM)
        vmem = pl.BlockSpec(memory_space=pltpu.VMEM)
        spectra, gram_parts = pl.pallas_call(
            functools.partial(exchange_kernel, groups, width, cores, depth),
            name="exchange",
            out_shape=(
                jax.ShapeDtypeStruct((4, VARS, groups, 8, LANES), jnp.float32),
                jax.ShapeDtypeStruct((groups, 1, LANES), jnp.float32),
            ),
            in_specs=[hbm, hbm, hbm],
            out_specs=(vmem, vmem),
            scratch_shapes=[
                pltpu.VMEM((VARS, steps, points), jnp.bfloat16),
                pltpu.VMEM((VARS, groups, steps, width), jnp.bfloat16),
                pltpu.VMEM((ROWS, RECORD_LENGTH), jnp.float32),
                pltpu.VMEM((ROWS, RECORD_LENGTH), jnp.bfloat16),
                pltpu.VMEM((ROWS, width), jnp.float32),
                pltpu.VMEM((ROWS * width // LANES, LANES), jnp.float32),
                pltpu.VMEM((VARS, groups, 4, 8, LANES), jnp.bfloat16),
                pltpu.VMEM((VARS, groups, 4, 8, LANES), jnp.bfloat16),
                pltpu.VMEM((points // LANES, LANES), jnp.float32),
                pltpu.VMEM((2 * points // LANES, LANES), jnp.float32),
                pltpu.SMEM((RETAINED_MODES,), jnp.int32),
                pltpu.VMEM((4, RETAINED_MODES, LANES), jnp.float32),
                pltpu.VMEM((1, LANES), jnp.float32),
                pltpu.VMEM((cores * depth, 1, LANES), jnp.float32),
                pltpu.VMEM((1, LANES), jnp.float32),
                pltpu.SemaphoreType.DMA((VARS,)),
                pltpu.SemaphoreType.DMA((VARS,)),
                pltpu.SemaphoreType.DMA((2,)),
                pltpu.SemaphoreType.DMA((VARS,)),
                pltpu.SemaphoreType.DMA((VARS,)),
                pltpu.SemaphoreType.DMA((VARS,)),
                pltpu.SemaphoreType.DMA((VARS,)),
                pltpu.SemaphoreType.DMA,
                pltpu.SemaphoreType.DMA,
                pltpu.SemaphoreType.DMA,
                pltpu.SemaphoreType.DMA,
                pltpu.SemaphoreType.REGULAR((4,)),
                pltpu.SemaphoreType.REGULAR,
                pltpu.SemaphoreType.REGULAR,
                pltpu.VMEM((groups, steps, BORROWED), jnp.bfloat16),
                pltpu.SemaphoreType.DMA((4,)),
            ],
            compiler_params=pltpu.CompilerParams(collective_id=0, has_side_effects=True, vmem_limit_bytes=32 * 2**20),
        )(*(pltpu.with_memory_space_constraint(a, pltpu.HBM) for a in (series, weights, spectral_indices)))
        total = points * cores * depth * VARS
        spectra, gram = pl.pallas_call(
            functools.partial(finish_kernel, total),
            name="finish",
            out_shape=(
                jax.ShapeDtypeStruct((4, VARS, groups, 8, LANES), jnp.float32),
                jax.ShapeDtypeStruct((2, 2, 2, 2), jnp.float32),
            ),
            in_specs=[vmem, vmem],
            out_specs=(hbm, hbm),
            scratch_shapes=[pltpu.VMEM((2, 2, 2, 2), jnp.float32), pltpu.SemaphoreType.DMA((5,))],
            compiler_params=pltpu.CompilerParams(vmem_limit_bytes=8 * 2**20),
        )(spectra, gram_parts)
        spectra = spectra.reshape(2, SEGMENT_NUMBER, VARS, groups, width // LANES, 2, LANES)
        spectra = spectra.transpose(0, 1, 5, 2, 3, 4, 6).reshape(2, SEGMENT_NUMBER, 2, VARS, points)
        return (spectra, gram)

    return jax.shard_map(
        on_device,
        mesh=mesh,
        in_specs=(P("ta", None, ("px", "py")), P(("px", "py")), P()),
        out_specs=(P("ta", None, None, None, ("px", "py")), P("ta", None, None, None)),
        check_vma=False,
    )
```

```python
import functools
import math

import jax
import jax.numpy as jnp
from jax import lax
from jax.experimental import pallas as pl
from jax.experimental.pallas import tpu as pltpu
from jax.sharding import PartitionSpec as P

VARS = 5
BLK = 256
HOP = 128
SEGMENT_NUMBER = 2
RECORD_LENGTH = 384
RETAINED_MODES = 32
ROWS = RETAINED_MODES * SEGMENT_NUMBER * 2
MESH = pl.DeviceIdType.MESH
LANES = 128
BORROWED = 128
STEPS = (
    (0, 1), (0, 3), (1, 0), (3, 0), (0, 2), (2, 0), (1, 1), (3, 3),
    (1, 3), (3, 1), (2, 1), (2, 3), (1, 2), (3, 2), (2, 2),
)
NEAR, SECOND, THIRD = slice(0, 4), slice(4, 10), slice(10, 14)


def cosine(phase):
    k = jnp.bitwise_and(phase, BLK - 1)
    k = jnp.where(k > BLK // 2, BLK - k, k)
    far = k > BLK // 4
    k = jnp.where(far, BLK // 2 - k, k)
    a = k.astype(jnp.float32) * jnp.float32(2.0 * math.pi / BLK)
    s = a * a
    total = jnp.float32(1.0 / math.factorial(12))
    for n in (10, 8, 6, 4, 2, 0):
        total = total * s * -1.0 if n == 10 else total * s
        total = total + jnp.float32((-1.0) ** (n // 2) / math.factorial(n))
    return jnp.where(far, -total, total)


def exchange_kernel(
    groups, width, cores, depth,
    snap, weights, indices, spectra, gram_out,
    mine, arrived, multipliers, twiddles, terms, turned, staged, held, w_ref, roots, idx_ref, sums, gram_mine, gram_seen, gram_sum,
    load_sem, own_sem, small_sem, send_sem, recv_sem, send_two, recv_two, gram_send, gram_recv, last_send, last_recv, known, here, everyone, relay, relay_sem,
):
    me = lax.axis_index("ta")
    side = math.isqrt(groups)
    y, x = me // side, me % side

    def member(step):
        return lax.rem(y + step[0], side) * side + lax.rem(x + step[1], side)

    barrier = pltpu.get_barrier_semaphore()
    peers = [member(step) for step in STEPS[NEAR]]
    for peer in peers:
        pl.semaphore_signal(barrier, inc=1, device_id={"ta": peer}, device_id_type=MESH)
    loads = [pltpu.make_async_copy(snap.at[v], mine.at[v], load_sem.at[v]) for v in range(VARS)]
    for load in loads:
        load.start()
    px, py = lax.axis_index("px"), lax.axis_index("py")
    late, partner = py >= depth // 2, depth - 1 - py
    last = VARS - 1
    place = px * depth + py
    others = [(dp, dz) for dz in range(depth) for dp in range(cores) if (dp, dz) != (0, 0)]

    @pl.when(place == 0)
    def _():
        for p, z in others:
            pl.semaphore_signal(barrier, inc=1, device_id={"px": p, "py": z}, device_id_type=MESH)

    @pl.when(jnp.logical_not(late))
    def _():
        pl.semaphore_signal(barrier, inc=1, device_id={"py": partner}, device_id_type=MESH)

    peers += [member(step) for step in STEPS[NEAR.stop :]]
    planes = [(lax.rem(px + dp, cores), lax.rem(py + dz, depth)) for dp, dz in others]
    far_planes = [planes[i] for i in sorted(range(len(others)), key=lambda i: -min(others[i][1], depth - others[i][1]))]
    n, n_planes, tiles = len(peers), len(planes), width // LANES
    index_copy = pltpu.make_async_copy(indices, idx_ref, small_sem.at[0])
    index_copy.start()
    weight_copy = pltpu.make_async_copy(weights, w_ref, small_sem.at[1])
    weight_copy.start()
    own = pl.ds(pl.multiple_of(me * width, LANES), width)
    kept = pl.ds(BORROWED, width - BORROWED)
    for v in range(last):
        pltpu.make_async_copy(snap.at[v, :, own], arrived.at[v, me], own_sem.at[v]).start()

    def own_last():
        cut = pl.ds(pl.multiple_of(me * width + BORROWED, LANES), width - BORROWED)
        return pltpu.make_async_copy(snap.at[last, :, cut], arrived.at[last, me, :, kept], own_sem.at[last])

    def own_whole(v):
        return pltpu.make_async_copy(snap.at[v, :, own], arrived.at[v, me], own_sem.at[v])

    @pl.when(late)
    def _():
        own_last().start()

    @pl.when(jnp.logical_not(late))
    def _():
        own_whole(last).start()

    pl.semaphore_wait(barrier, jnp.where(place == 0, 4, jnp.where(late, 6, 5)))

    def tell(i):
        for peer in peers[NEAR]:
            pl.semaphore_signal(known.at[i], inc=1, device_id={"ta": peer}, device_id_type=MESH)

    def send(v, to):
        for peer in to:
            cut = pl.ds(pl.multiple_of(peer * width, LANES), width)
            pltpu.make_async_remote_copy(
                src_ref=mine.at[v, :, cut], dst_ref=arrived.at[v, me], send_sem=send_sem.at[v], recv_sem=recv_sem.at[v],
                device_id={"ta": peer}, device_id_type=MESH,
            ).start()

    def send_each(to):
        def step(v, carry):
            send(v, to)
            return carry

        return step

    tell(0)

    @pl.when(place != 0)
    def _():
        pl.semaphore_signal(here, inc=1, device_id={"px": 0, "py": 0}, device_id_type=MESH)

    for v in range(VARS - 1):
        loads[v].wait()
        send(v, peers[NEAR])
    loads[VARS - 1].wait()
    pl.semaphore_wait(known.at[0], 4)
    tell(1)
    lax.fori_loop(0, VARS - 1, send_each(peers[SECOND]), 0)
    pl.semaphore_wait(known.at[1], 4)
    tell(2)
    send(0, peers[THIRD])
    pl.semaphore_wait(known.at[2], 4)
    tell(3)
    send(0, peers[14:])
    pl.semaphore_wait(known.at[3], 4)

    @pl.when(late)
    def _():
        for peer in [*peers[::-1], me]:
            cut = pl.ds(pl.multiple_of(peer * width, LANES), BORROWED)
            pltpu.make_async_remote_copy(
                src_ref=mine.at[last, :, cut], dst_ref=relay.at[me], send_sem=relay_sem.at[0], recv_sem=relay_sem.at[1],
                device_id={"ta": peer, "py": partner}, device_id_type=MESH,
            ).start()

    lax.fori_loop(1, VARS - 1, send_each(peers[10:]), 0)

    @pl.when(late)
    def _():
        for peer in peers[::-1]:
            cut = pl.ds(pl.multiple_of(peer * width + BORROWED, LANES), width - BORROWED)
            pltpu.make_async_remote_copy(
                src_ref=mine.at[last, :, cut], dst_ref=arrived.at[last, me, :, kept],
                send_sem=send_sem.at[last], recv_sem=recv_sem.at[last],
                device_id={"ta": peer}, device_id_type=MESH,
            ).start()

    @pl.when(jnp.logical_not(late))
    def _():
        send(last, peers[::-1])

    index_copy.wait()
    shape = (8, RECORD_LENGTH)
    row = lax.broadcasted_iota(jnp.int32, shape, 0)
    time = lax.broadcasted_iota(jnp.int32, shape, 1)
    windows = []
    for b in range(SEGMENT_NUMBER):
        lag = time - HOP * b
        window = jnp.float32(0.5) - jnp.float32(0.5) * cosine(lag)
        window = jnp.where((lag >= 0) & (lag < BLK), window, jnp.float32(0.0))
        windows.append(window / jnp.sqrt(jnp.float32(3.0 * BLK / 8.0)))

    def fill(g, carry):
        index = jnp.full(shape, idx_ref[8 * g], jnp.int32)
        for i in range(1, 8):
            index = jnp.where(row == i, idx_ref[8 * g + i], index)
        for b in range(SEGMENT_NUMBER):
            phase = index * (time - HOP * b)
            for c in range(2):
                rows = pl.ds(pl.multiple_of(64 * c + 32 * b + 8 * g, 8), 8)
                multipliers[rows, :] = cosine(phase + (BLK // 4) * c) * windows[b]
        return carry

    lax.fori_loop(0, RETAINED_MODES // 8, fill, 0)
    twiddles[...] = multipliers[...].astype(jnp.bfloat16)
    sums[...] = jnp.zeros_like(sums)
    weight_copy.wait()
    root = jnp.sqrt(w_ref[...])
    for c in range(2):
        roots[pl.ds(c, groups * tiles, stride=2), :] = root

    @pl.when(place == 0)
    def _():
        pl.semaphore_wait(here, n_planes)
        for p, z in others:
            pl.semaphore_signal(everyone, inc=1, device_id={"px": p, "py": z}, device_id_type=MESH)

    def arrive(v):
        pltpu.make_async_copy(arrived.at[v, pl.ds(0, n)], arrived.at[v, pl.ds(0, n)], recv_sem.at[v]).wait()
        own_whole(v).wait()

    def parts_of_last():
        return arrived.at[last, pl.ds(0, n), :, kept]

    def transform(v):
        series = arrived[v].reshape(RECORD_LENGTH, width)
        raw = jnp.dot(twiddles[...], series, preferred_element_type=jnp.float32)
        terms[...] = raw
        total = [sums[i] for i in range(4)]
        for j in range(tiles):
            w = w_ref[pl.ds(me * tiles + j, 1), :]
            cut = slice(j * LANES, (j + 1) * LANES)
            r0, r1, i0, i1 = (terms[32 * i : 32 * i + 32, cut] for i in range(4))
            total[0] += (r0 * r0 + i0 * i0) * w
            total[1] += (r1 * r1 + i1 * i1) * w
            total[2] += (r0 * r1 + i0 * i1) * w
            total[3] += (r0 * i1 - i0 * r1) * w
        for i in range(4):
            sums[i] = total[i]

    def lay_out(v):
        for j in range(tiles):
            for b in range(SEGMENT_NUMBER):
                for c in range(2):
                    first = 64 * c + 32 * b
                    part = terms[first : first + RETAINED_MODES, j * LANES : (j + 1) * LANES]
                    turned[pl.ds(8 * b + 2 * j + c, RETAINED_MODES, stride=16), :] = part
        staged[v] = turned[...].astype(jnp.bfloat16).reshape(groups, 4, 8, LANES)
        held[v, me] = staged[v, me]

    def send_back(v):
        for peer in peers[::-1]:
            pltpu.make_async_remote_copy(
                src_ref=staged.at[v, peer], dst_ref=held.at[v, me], send_sem=send_two.at[v], recv_sem=recv_two.at[v],
                device_id={"ta": peer}, device_id_type=MESH,
            ).start()

    def work(v, carry):
        arrive(v)
        transform(v)
        lay_out(v)
        return carry

    @pl.when(jnp.logical_not(late))
    def _():
        pltpu.make_async_copy(relay, relay, relay_sem.at[1]).wait()
        pltpu.make_async_remote_copy(
            src_ref=relay, dst_ref=arrived.at[last, :, :, pl.ds(0, BORROWED)],
            send_sem=relay_sem.at[2], recv_sem=relay_sem.at[3],
            device_id={"py": partner}, device_id_type=MESH,
        ).start()

    lax.fori_loop(0, VARS - 1, work, 0)

    @pl.when(late)
    def _():
        own_last().wait()
        pltpu.make_async_copy(parts_of_last(), parts_of_last(), recv_sem.at[last]).wait()
        pltpu.make_async_copy(relay, relay, relay_sem.at[3]).wait()

    @pl.when(jnp.logical_not(late))
    def _():
        arrive(last)

    def send_early(v, carry):
        send_back(v)
        return carry

    lax.fori_loop(0, 2, send_early, 0)
    transform(last)

    shape = (RETAINED_MODES, LANES)
    ahead = lax.broadcasted_iota(jnp.int32, shape, 1) - lax.broadcasted_iota(jnp.int32, shape, 0)
    lanes = jnp.zeros(shape, jnp.float32)
    for i in range(4):
        lanes = jnp.where(ahead == RETAINED_MODES * i, jnp.sum(sums[i], axis=1, keepdims=True), lanes)
    lanes = jnp.sum(lanes, axis=0, keepdims=True)
    gram_mine[...] = lanes
    gram_seen[place] = lanes

    @pl.when(place != 0)
    def _():
        pl.semaphore_wait(everyone, 1)

    for p, z in far_planes:
        pltpu.make_async_remote_copy(
            src_ref=gram_mine, dst_ref=gram_seen.at[place], send_sem=gram_send, recv_sem=gram_recv,
            device_id={"px": p, "py": z}, device_id_type=MESH,
        ).start()
    lax.fori_loop(2, VARS - 1, send_early, 0)
    lay_out(VARS - 1)
    send_back(VARS - 1)

    def scale(v, carry):
        pltpu.make_async_copy(held.at[v, pl.ds(0, n)], held.at[v, pl.ds(0, n)], recv_two.at[v]).wait()
        for k in range(groups):
            by = roots[8 * k : 8 * k + 8, :]
            for i in range(4):
                spectra[i, v, k] = held[v, k, i].astype(jnp.float32) * by
        return carry

    pltpu.make_async_copy(gram_seen.at[pl.ds(0, n_planes)], gram_seen.at[pl.ds(0, n_planes)], gram_recv).wait()
    whole = jnp.sum(gram_seen[...], axis=0)
    gram_sum[...] = whole
    gram_out[me] = whole
    for peer in peers[::-1]:
        pltpu.make_async_remote_copy(
            src_ref=gram_sum, dst_ref=gram_out.at[me], send_sem=last_send, recv_sem=last_recv,
            device_id={"ta": peer}, device_id_type=MESH,
        ).start()
    lax.fori_loop(0, VARS, scale, 0)
    pltpu.make_async_copy(gram_out.at[pl.ds(0, n)], gram_out.at[pl.ds(0, n)], last_recv).wait()
    for v in range(last):
        pltpu.make_async_copy(arrived.at[v, pl.ds(0, n)], arrived.at[v, pl.ds(0, n)], send_sem.at[v]).wait()

    @pl.when(late)
    def _():
        pltpu.make_async_copy(parts_of_last(), parts_of_last(), send_sem.at[last]).wait()
        pltpu.make_async_copy(relay, relay, relay_sem.at[0]).wait()

    @pl.when(jnp.logical_not(late))
    def _():
        pltpu.make_async_copy(arrived.at[last, pl.ds(0, n)], arrived.at[last, pl.ds(0, n)], send_sem.at[last]).wait()
        pltpu.make_async_copy(relay, relay, relay_sem.at[2]).wait()

    for v in range(VARS):
        pltpu.make_async_copy(held.at[v, pl.ds(0, n)], held.at[v, pl.ds(0, n)], send_two.at[v]).wait()
    pltpu.make_async_copy(gram_seen.at[pl.ds(0, n_planes)], gram_seen.at[pl.ds(0, n_planes)], gram_send).wait()
    pltpu.make_async_copy(gram_out.at[pl.ds(0, n)], gram_out.at[pl.ds(0, n)], last_send).wait()


def finish_kernel(total, spectra, gram_in, out, gram_out, gram, sem):
    copies = [pltpu.make_async_copy(spectra.at[i], out.at[i], sem.at[i]) for i in range(4)]
    for copy in copies:
        copy.start()
    me = lax.axis_index("ta")
    sums = jnp.sum(gram_in[...], axis=0) / jnp.float32(total)
    sums = pltpu.roll(sums, lax.rem(LANES - 2 * me, LANES), 1)
    r = lax.broadcasted_iota(jnp.int32, (2, 2), 0)
    c = lax.broadcasted_iota(jnp.int32, (2, 2), 1)
    zero = jnp.zeros((2, 2), jnp.float32)
    for f in range(2):
        first, second, real, imag = (jnp.broadcast_to(sums[:, RETAINED_MODES * i + f : RETAINED_MODES * i + f + 1], (2, 2)) for i in range(4))
        for b in range(2):
            power = jnp.where(c == 0, second if b else first, zero)
            gram[f, b] = jnp.where(r == b, power, jnp.where(c == 0, real, -imag if b else imag))
    copies.append(pltpu.make_async_copy(gram, gram_out, sem.at[4]))
    copies[-1].start()
    for copy in copies:
        copy.wait()


def solution(mesh):
    groups, cores, depth = mesh.shape["ta"], mesh.shape["px"], mesh.shape["py"]

    def on_device(snapshots, quad_weights, spectral_indices):
        steps, _, points = snapshots.shape
        width = points // groups
        series = jnp.transpose(snapshots, (1, 0, 2))
        weights = quad_weights.reshape(points // LANES, LANES)
        hbm = pl.BlockSpec(memory_space=pltpu.HBM)
        vmem = pl.BlockSpec(memory_space=pltpu.VMEM)
        spectra, gram_parts = pl.pallas_call(
            functools.partial(exchange_kernel, groups, width, cores, depth),
            name="exchange",
            out_shape=(
                jax.ShapeDtypeStruct((4, VARS, groups, 8, LANES), jnp.float32),
                jax.ShapeDtypeStruct((groups, 1, LANES), jnp.float32),
            ),
            in_specs=[hbm, hbm, hbm],
            out_specs=(vmem, vmem),
            scratch_shapes=[
                pltpu.VMEM((VARS, steps, points), jnp.bfloat16),
                pltpu.VMEM((VARS, groups, steps, width), jnp.bfloat16),
                pltpu.VMEM((ROWS, RECORD_LENGTH), jnp.float32),
                pltpu.VMEM((ROWS, RECORD_LENGTH), jnp.bfloat16),
                pltpu.VMEM((ROWS, width), jnp.float32),
                pltpu.VMEM((ROWS * width // LANES, LANES), jnp.float32),
                pltpu.VMEM((VARS, groups, 4, 8, LANES), jnp.bfloat16),
                pltpu.VMEM((VARS, groups, 4, 8, LANES), jnp.bfloat16),
                pltpu.VMEM((points // LANES, LANES), jnp.float32),
                pltpu.VMEM((2 * points // LANES, LANES), jnp.float32),
                pltpu.SMEM((RETAINED_MODES,), jnp.int32),
                pltpu.VMEM((4, RETAINED_MODES, LANES), jnp.float32),
                pltpu.VMEM((1, LANES), jnp.float32),
                pltpu.VMEM((cores * depth, 1, LANES), jnp.float32),
                pltpu.VMEM((1, LANES), jnp.float32),
                pltpu.SemaphoreType.DMA((VARS,)),
                pltpu.SemaphoreType.DMA((VARS,)),
                pltpu.SemaphoreType.DMA((2,)),
                pltpu.SemaphoreType.DMA((VARS,)),
                pltpu.SemaphoreType.DMA((VARS,)),
                pltpu.SemaphoreType.DMA((VARS,)),
                pltpu.SemaphoreType.DMA((VARS,)),
                pltpu.SemaphoreType.DMA,
                pltpu.SemaphoreType.DMA,
                pltpu.SemaphoreType.DMA,
                pltpu.SemaphoreType.DMA,
                pltpu.SemaphoreType.REGULAR((4,)),
                pltpu.SemaphoreType.REGULAR,
                pltpu.SemaphoreType.REGULAR,
                pltpu.VMEM((groups, steps, BORROWED), jnp.bfloat16),
                pltpu.SemaphoreType.DMA((4,)),
            ],
            compiler_params=pltpu.CompilerParams(collective_id=0, has_side_effects=True, vmem_limit_bytes=32 * 2**20),
        )(*(pltpu.with_memory_space_constraint(a, pltpu.HBM) for a in (series, weights, spectral_indices)))
        total = points * cores * depth * VARS
        spectra, gram = pl.pallas_call(
            functools.partial(finish_kernel, total),
            name="finish",
            out_shape=(
                jax.ShapeDtypeStruct((4, VARS, groups, 8, LANES), jnp.float32),
                jax.ShapeDtypeStruct((2, 2, 2, 2), jnp.float32),
            ),
            in_specs=[vmem, vmem],
            out_specs=(hbm, hbm),
            scratch_shapes=[pltpu.VMEM((2, 2, 2, 2), jnp.float32), pltpu.SemaphoreType.DMA((5,))],
            compiler_params=pltpu.CompilerParams(vmem_limit_bytes=8 * 2**20),
        )(spectra, gram_parts)
        spectra = spectra.reshape(2, SEGMENT_NUMBER, VARS, groups, width // LANES, 2, LANES)
        spectra = spectra.transpose(0, 1, 5, 2, 3, 4, 6).reshape(2, SEGMENT_NUMBER, 2, VARS, points)
        return (spectra, gram)

    return jax.shard_map(
        on_device,
        mesh=mesh,
        in_specs=(P("ta", None, ("px", "py")), P(("px", "py")), P()),
        out_specs=(P("ta", None, None, None, ("px", "py")), P("ta", None, None, None)),
        check_vma=False,
    )
```

```python
import functools
import math

import jax
import jax.numpy as jnp
from jax import lax
from jax.experimental import pallas as pl
from jax.experimental.pallas import tpu as pltpu
from jax.sharding import PartitionSpec as P

VARS = 5
BLK = 256
HOP = 128
SEGMENT_NUMBER = 2
RECORD_LENGTH = 384
RETAINED_MODES = 32
ROWS = RETAINED_MODES * SEGMENT_NUMBER * 2
MESH = pl.DeviceIdType.MESH
LANES = 128
BORROWED = 128
STEPS = (
    (0, 1), (0, 3), (1, 0), (3, 0), (0, 2), (2, 0), (1, 1), (3, 3),
    (1, 3), (3, 1), (2, 1), (2, 3), (1, 2), (3, 2), (2, 2),
)
NEAR, SECOND, THIRD = slice(0, 4), slice(4, 10), slice(10, 14)


def cosine(phase):
    k = jnp.bitwise_and(phase, BLK - 1)
    k = jnp.where(k > BLK // 2, BLK - k, k)
    far = k > BLK // 4
    k = jnp.where(far, BLK // 2 - k, k)
    a = k.astype(jnp.float32) * jnp.float32(2.0 * math.pi / BLK)
    s = a * a
    total = jnp.float32(1.0 / math.factorial(12))
    for n in (10, 8, 6, 4, 2, 0):
        total = total * s * -1.0 if n == 10 else total * s
        total = total + jnp.float32((-1.0) ** (n // 2) / math.factorial(n))
    return jnp.where(far, -total, total)


def exchange_kernel(
    groups, width, cores, depth,
    snap, weights, indices, spectra, gram_out,
    mine, arrived, multipliers, twiddles, terms, turned, staged, held, w_ref, roots, idx_ref, sums, gram_mine, gram_seen, gram_sum,
    load_sem, own_sem, small_sem, send_sem, recv_sem, send_two, recv_two, gram_send, gram_recv, last_send, last_recv, known, here, everyone, relay, relay_sem,
):
    me = lax.axis_index("ta")
    side = math.isqrt(groups)
    y, x = me // side, me % side

    def member(step):
        return lax.rem(y + step[0], side) * side + lax.rem(x + step[1], side)

    barrier = pltpu.get_barrier_semaphore()
    peers = [member(step) for step in STEPS[NEAR]]
    for peer in peers:
        pl.semaphore_signal(barrier, inc=1, device_id={"ta": peer}, device_id_type=MESH)
    loads = [pltpu.make_async_copy(snap.at[v], mine.at[v], load_sem.at[v]) for v in range(VARS)]
    for load in loads:
        load.start()
    px, py = lax.axis_index("px"), lax.axis_index("py")
    late, partner = py >= depth // 2, depth - 1 - py
    last = VARS - 1
    place = px * depth + py
    others = [(dp, dz) for dz in range(depth) for dp in range(cores) if (dp, dz) != (0, 0)]

    @pl.when(place == 0)
    def _():
        for p, z in others:
            pl.semaphore_signal(barrier, inc=1, device_id={"px": p, "py": z}, device_id_type=MESH)

    @pl.when(jnp.logical_not(late))
    def _():
        pl.semaphore_signal(barrier, inc=1, device_id={"py": partner}, device_id_type=MESH)

    peers += [member(step) for step in STEPS[NEAR.stop :]]
    planes = [(lax.rem(px + dp, cores), lax.rem(py + dz, depth)) for dp, dz in others]
    far_planes = [planes[i] for i in sorted(range(len(others)), key=lambda i: -min(others[i][1], depth - others[i][1]))]
    n, n_planes, tiles = len(peers), len(planes), width // LANES
    index_copy = pltpu.make_async_copy(indices, idx_ref, small_sem.at[0])
    index_copy.start()
    weight_copy = pltpu.make_async_copy(weights, w_ref, small_sem.at[1])
    weight_copy.start()
    own = pl.ds(pl.multiple_of(me * width, LANES), width)
    kept = pl.ds(BORROWED, width - BORROWED)
    for v in range(last):
        pltpu.make_async_copy(snap.at[v, :, own], arrived.at[v, me], own_sem.at[v]).start()

    def own_last():
        cut = pl.ds(pl.multiple_of(me * width + BORROWED, LANES), width - BORROWED)
        return pltpu.make_async_copy(snap.at[last, :, cut], arrived.at[last, me, :, kept], own_sem.at[last])

    def own_whole(v):
        return pltpu.make_async_copy(snap.at[v, :, own], arrived.at[v, me], own_sem.at[v])

    @pl.when(late)
    def _():
        own_last().start()

    @pl.when(jnp.logical_not(late))
    def _():
        own_whole(last).start()

    pl.semaphore_wait(barrier, jnp.where(place == 0, 4, jnp.where(late, 6, 5)))

    def tell(i):
        for peer in peers[NEAR]:
            pl.semaphore_signal(known.at[i], inc=1, device_id={"ta": peer}, device_id_type=MESH)

    def send(v, to):
        for peer in to:
            cut = pl.ds(pl.multiple_of(peer * width, LANES), width)
            pltpu.make_async_remote_copy(
                src_ref=mine.at[v, :, cut], dst_ref=arrived.at[v, me], send_sem=send_sem.at[v], recv_sem=recv_sem.at[v],
                device_id={"ta": peer}, device_id_type=MESH,
            ).start()

    def send_each(to):
        def step(v, carry):
            send(v, to)
            return carry

        return step

    tell(0)

    @pl.when(place != 0)
    def _():
        pl.semaphore_signal(here, inc=1, device_id={"px": 0, "py": 0}, device_id_type=MESH)

    for v in range(VARS - 1):
        loads[v].wait()
        send(v, peers[NEAR])
    loads[VARS - 1].wait()
    pl.semaphore_wait(known.at[0], 4)
    tell(1)
    lax.fori_loop(0, VARS - 1, send_each(peers[SECOND]), 0)
    pl.semaphore_wait(known.at[1], 4)
    tell(2)
    send(0, peers[THIRD])
    pl.semaphore_wait(known.at[2], 4)
    tell(3)
    send(0, peers[14:])
    pl.semaphore_wait(known.at[3], 4)

    @pl.when(late)
    def _():
        for peer in [*peers[::-1], me]:
            cut = pl.ds(pl.multiple_of(peer * width, LANES), BORROWED)
            pltpu.make_async_remote_copy(
                src_ref=mine.at[last, :, cut], dst_ref=relay.at[me], send_sem=relay_sem.at[0], recv_sem=relay_sem.at[1],
                device_id={"ta": peer, "py": partner}, device_id_type=MESH,
            ).start()

    lax.fori_loop(1, VARS - 1, send_each(peers[10:]), 0)

    @pl.when(late)
    def _():
        for peer in peers[::-1]:
            cut = pl.ds(pl.multiple_of(peer * width + BORROWED, LANES), width - BORROWED)
            pltpu.make_async_remote_copy(
                src_ref=mine.at[last, :, cut], dst_ref=arrived.at[last, me, :, kept],
                send_sem=send_sem.at[last], recv_sem=recv_sem.at[last],
                device_id={"ta": peer}, device_id_type=MESH,
            ).start()

    @pl.when(jnp.logical_not(late))
    def _():
        send(last, peers[::-1])

    index_copy.wait()
    shape = (8, RECORD_LENGTH)
    row = lax.broadcasted_iota(jnp.int32, shape, 0)
    time = lax.broadcasted_iota(jnp.int32, shape, 1)
    windows = []
    for b in range(SEGMENT_NUMBER):
        lag = time - HOP * b
        window = jnp.float32(0.5) - jnp.float32(0.5) * cosine(lag)
        window = jnp.where((lag >= 0) & (lag < BLK), window, jnp.float32(0.0))
        windows.append(window / jnp.sqrt(jnp.float32(3.0 * BLK / 8.0)))

    def fill(g, carry):
        index = jnp.full(shape, idx_ref[8 * g], jnp.int32)
        for i in range(1, 8):
            index = jnp.where(row == i, idx_ref[8 * g + i], index)
        for b in range(SEGMENT_NUMBER):
            phase = index * (time - HOP * b)
            for c in range(2):
                rows = pl.ds(pl.multiple_of(64 * c + 32 * b + 8 * g, 8), 8)
                multipliers[rows, :] = cosine(phase + (BLK // 4) * c) * windows[b]
        return carry

    lax.fori_loop(0, RETAINED_MODES // 8, fill, 0)
    twiddles[...] = multipliers[...].astype(jnp.bfloat16)
    sums[...] = jnp.zeros_like(sums)
    weight_copy.wait()
    root = jnp.sqrt(w_ref[...])
    for c in range(2):
        roots[pl.ds(c, groups * tiles, stride=2), :] = root

    @pl.when(place == 0)
    def _():
        pl.semaphore_wait(here, n_planes)
        for p, z in others:
            pl.semaphore_signal(everyone, inc=1, device_id={"px": p, "py": z}, device_id_type=MESH)

    def arrive(v):
        pltpu.make_async_copy(arrived.at[v, pl.ds(0, n)], arrived.at[v, pl.ds(0, n)], recv_sem.at[v]).wait()
        own_whole(v).wait()

    def parts_of_last():
        return arrived.at[last, pl.ds(0, n), :, kept]

    def transform(v):
        series = arrived[v].reshape(RECORD_LENGTH, width)
        raw = jnp.dot(twiddles[...], series, preferred_element_type=jnp.float32)
        terms[...] = raw
        total = [sums[i] for i in range(4)]
        for j in range(tiles):
            w = w_ref[pl.ds(me * tiles + j, 1), :]
            cut = slice(j * LANES, (j + 1) * LANES)
            r0, r1, i0, i1 = (raw[32 * i : 32 * i + 32, cut] for i in range(4))
            total[0] += (r0 * r0 + i0 * i0) * w
            total[1] += (r1 * r1 + i1 * i1) * w
            total[2] += (r0 * r1 + i0 * i1) * w
            total[3] += (r0 * i1 - i0 * r1) * w
        for i in range(4):
            sums[i] = total[i]

    def lay_out(v):
        for j in range(tiles):
            for b in range(SEGMENT_NUMBER):
                for c in range(2):
                    first = 64 * c + 32 * b
                    part = terms[first : first + RETAINED_MODES, j * LANES : (j + 1) * LANES]
                    turned[pl.ds(8 * b + 2 * j + c, RETAINED_MODES, stride=16), :] = part
        staged[v] = turned[...].astype(jnp.bfloat16).reshape(groups, 4, 8, LANES)
        held[v, me] = staged[v, me]

    def send_back(v):
        for peer in peers[::-1]:
            pltpu.make_async_remote_copy(
                src_ref=staged.at[v, peer], dst_ref=held.at[v, me], send_sem=send_two.at[v], recv_sem=recv_two.at[v],
                device_id={"ta": peer}, device_id_type=MESH,
            ).start()

    def work(v, carry):
        arrive(v)
        transform(v)
        lay_out(v)
        return carry

    @pl.when(jnp.logical_not(late))
    def _():
        pltpu.make_async_copy(relay, relay, relay_sem.at[1]).wait()
        pltpu.make_async_remote_copy(
            src_ref=relay, dst_ref=arrived.at[last, :, :, pl.ds(0, BORROWED)],
            send_sem=relay_sem.at[2], recv_sem=relay_sem.at[3],
            device_id={"py": partner}, device_id_type=MESH,
        ).start()

    lax.fori_loop(0, VARS - 1, work, 0)

    @pl.when(late)
    def _():
        own_last().wait()
        pltpu.make_async_copy(parts_of_last(), parts_of_last(), recv_sem.at[last]).wait()
        pltpu.make_async_copy(relay, relay, relay_sem.at[3]).wait()

    @pl.when(jnp.logical_not(late))
    def _():
        arrive(last)

    def send_early(v, carry):
        send_back(v)
        return carry

    lax.fori_loop(0, VARS - 1, send_early, 0)
    transform(last)

    shape = (RETAINED_MODES, LANES)
    ahead = lax.broadcasted_iota(jnp.int32, shape, 1) - lax.broadcasted_iota(jnp.int32, shape, 0)
    lanes = jnp.zeros(shape, jnp.float32)
    for i in range(4):
        lanes = jnp.where(ahead == RETAINED_MODES * i, jnp.sum(sums[i], axis=1, keepdims=True), lanes)
    lanes = jnp.sum(lanes, axis=0, keepdims=True)
    gram_mine[...] = lanes
    gram_seen[place] = lanes

    @pl.when(place != 0)
    def _():
        pl.semaphore_wait(everyone, 1)

    for p, z in far_planes:
        pltpu.make_async_remote_copy(
            src_ref=gram_mine, dst_ref=gram_seen.at[place], send_sem=gram_send, recv_sem=gram_recv,
            device_id={"px": p, "py": z}, device_id_type=MESH,
        ).start()
    lay_out(VARS - 1)
    send_back(VARS - 1)

    def scale(v, carry):
        pltpu.make_async_copy(held.at[v, pl.ds(0, n)], held.at[v, pl.ds(0, n)], recv_two.at[v]).wait()
        for k in range(groups):
            by = roots[8 * k : 8 * k + 8, :]
            for i in range(4):
                spectra[i, v, k] = held[v, k, i].astype(jnp.float32) * by
        return carry

    pltpu.make_async_copy(gram_seen.at[pl.ds(0, n_planes)], gram_seen.at[pl.ds(0, n_planes)], gram_recv).wait()
    whole = jnp.sum(gram_seen[...], axis=0)
    gram_sum[...] = whole
    gram_out[me] = whole
    for peer in peers[::-1]:
        pltpu.make_async_remote_copy(
            src_ref=gram_sum, dst_ref=gram_out.at[me], send_sem=last_send, recv_sem=last_recv,
            device_id={"ta": peer}, device_id_type=MESH,
        ).start()
    lax.fori_loop(0, VARS, scale, 0)
    pltpu.make_async_copy(gram_out.at[pl.ds(0, n)], gram_out.at[pl.ds(0, n)], last_recv).wait()
    for v in range(last):
        pltpu.make_async_copy(arrived.at[v, pl.ds(0, n)], arrived.at[v, pl.ds(0, n)], send_sem.at[v]).wait()

    @pl.when(late)
    def _():
        pltpu.make_async_copy(parts_of_last(), parts_of_last(), send_sem.at[last]).wait()
        pltpu.make_async_copy(relay, relay, relay_sem.at[0]).wait()

    @pl.when(jnp.logical_not(late))
    def _():
        pltpu.make_async_copy(arrived.at[last, pl.ds(0, n)], arrived.at[last, pl.ds(0, n)], send_sem.at[last]).wait()
        pltpu.make_async_copy(relay, relay, relay_sem.at[2]).wait()

    for v in range(VARS):
        pltpu.make_async_copy(held.at[v, pl.ds(0, n)], held.at[v, pl.ds(0, n)], send_two.at[v]).wait()
    pltpu.make_async_copy(gram_seen.at[pl.ds(0, n_planes)], gram_seen.at[pl.ds(0, n_planes)], gram_send).wait()
    pltpu.make_async_copy(gram_out.at[pl.ds(0, n)], gram_out.at[pl.ds(0, n)], last_send).wait()


def finish_kernel(total, spectra, gram_in, out, gram_out, gram, sem):
    copies = [pltpu.make_async_copy(spectra.at[i], out.at[i], sem.at[i]) for i in range(4)]
    for copy in copies:
        copy.start()
    me = lax.axis_index("ta")
    sums = jnp.sum(gram_in[...], axis=0) / jnp.float32(total)
    sums = pltpu.roll(sums, lax.rem(LANES - 2 * me, LANES), 1)
    r = lax.broadcasted_iota(jnp.int32, (2, 2), 0)
    c = lax.broadcasted_iota(jnp.int32, (2, 2), 1)
    zero = jnp.zeros((2, 2), jnp.float32)
    for f in range(2):
        first, second, real, imag = (jnp.broadcast_to(sums[:, RETAINED_MODES * i + f : RETAINED_MODES * i + f + 1], (2, 2)) for i in range(4))
        for b in range(2):
            power = jnp.where(c == 0, second if b else first, zero)
            gram[f, b] = jnp.where(r == b, power, jnp.where(c == 0, real, -imag if b else imag))
    copies.append(pltpu.make_async_copy(gram, gram_out, sem.at[4]))
    copies[-1].start()
    for copy in copies:
        copy.wait()


def solution(mesh):
    groups, cores, depth = mesh.shape["ta"], mesh.shape["px"], mesh.shape["py"]

    def on_device(snapshots, quad_weights, spectral_indices):
        steps, _, points = snapshots.shape
        width = points // groups
        series = jnp.transpose(snapshots, (1, 0, 2))
        weights = quad_weights.reshape(points // LANES, LANES)
        hbm = pl.BlockSpec(memory_space=pltpu.HBM)
        vmem = pl.BlockSpec(memory_space=pltpu.VMEM)
        spectra, gram_parts = pl.pallas_call(
            functools.partial(exchange_kernel, groups, width, cores, depth),
            name="exchange",
            out_shape=(
                jax.ShapeDtypeStruct((4, VARS, groups, 8, LANES), jnp.float32),
                jax.ShapeDtypeStruct((groups, 1, LANES), jnp.float32),
            ),
            in_specs=[hbm, hbm, hbm],
            out_specs=(vmem, vmem),
            scratch_shapes=[
                pltpu.VMEM((VARS, steps, points), jnp.bfloat16),
                pltpu.VMEM((VARS, groups, steps, width), jnp.bfloat16),
                pltpu.VMEM((ROWS, RECORD_LENGTH), jnp.float32),
                pltpu.VMEM((ROWS, RECORD_LENGTH), jnp.bfloat16),
                pltpu.VMEM((ROWS, width), jnp.float32),
                pltpu.VMEM((ROWS * width // LANES, LANES), jnp.float32),
                pltpu.VMEM((VARS, groups, 4, 8, LANES), jnp.bfloat16),
                pltpu.VMEM((VARS, groups, 4, 8, LANES), jnp.bfloat16),
                pltpu.VMEM((points // LANES, LANES), jnp.float32),
                pltpu.VMEM((2 * points // LANES, LANES), jnp.float32),
                pltpu.SMEM((RETAINED_MODES,), jnp.int32),
                pltpu.VMEM((4, RETAINED_MODES, LANES), jnp.float32),
                pltpu.VMEM((1, LANES), jnp.float32),
                pltpu.VMEM((cores * depth, 1, LANES), jnp.float32),
                pltpu.VMEM((1, LANES), jnp.float32),
                pltpu.SemaphoreType.DMA((VARS,)),
                pltpu.SemaphoreType.DMA((VARS,)),
                pltpu.SemaphoreType.DMA((2,)),
                pltpu.SemaphoreType.DMA((VARS,)),
                pltpu.SemaphoreType.DMA((VARS,)),
                pltpu.SemaphoreType.DMA((VARS,)),
                pltpu.SemaphoreType.DMA((VARS,)),
                pltpu.SemaphoreType.DMA,
                pltpu.SemaphoreType.DMA,
                pltpu.SemaphoreType.DMA,
                pltpu.SemaphoreType.DMA,
                pltpu.SemaphoreType.REGULAR((4,)),
                pltpu.SemaphoreType.REGULAR,
                pltpu.SemaphoreType.REGULAR,
                pltpu.VMEM((groups, steps, BORROWED), jnp.bfloat16),
                pltpu.SemaphoreType.DMA((4,)),
            ],
            compiler_params=pltpu.CompilerParams(collective_id=0, has_side_effects=True, vmem_limit_bytes=32 * 2**20),
        )(*(pltpu.with_memory_space_constraint(a, pltpu.HBM) for a in (series, weights, spectral_indices)))
        total = points * cores * depth * VARS
        spectra, gram = pl.pallas_call(
            functools.partial(finish_kernel, total),
            name="finish",
            out_shape=(
                jax.ShapeDtypeStruct((4, VARS, groups, 8, LANES), jnp.float32),
                jax.ShapeDtypeStruct((2, 2, 2, 2), jnp.float32),
            ),
            in_specs=[vmem, vmem],
            out_specs=(hbm, hbm),
            scratch_shapes=[pltpu.VMEM((2, 2, 2, 2), jnp.float32), pltpu.SemaphoreType.DMA((5,))],
            compiler_params=pltpu.CompilerParams(vmem_limit_bytes=8 * 2**20),
        )(spectra, gram_parts)
        spectra = spectra.reshape(2, SEGMENT_NUMBER, VARS, groups, width // LANES, 2, LANES)
        spectra = spectra.transpose(0, 1, 5, 2, 3, 4, 6).reshape(2, SEGMENT_NUMBER, 2, VARS, points)
        return (spectra, gram)

    return jax.shard_map(
        on_device,
        mesh=mesh,
        in_specs=(P("ta", None, ("px", "py")), P(("px", "py")), P()),
        out_specs=(P("ta", None, None, None, ("px", "py")), P("ta", None, None, None)),
        check_vma=False,
    )
```
